128 devices in a mesh: space: 16 (over x, z), ray: 8 (over y, core).
Axes of the slice: x: 4, y: 4, z: 4, core: 2. Of those that a mesh axis runs over, the one named last changes fastest.
Arguments:
- excite: float32 [2, 65536], P(None, ('space', 'ray')), may hold values from -6 to 6
- history: float32 [64, 65536], P(None, ('space', 'ray')), may hold values from -6 to 6
- near_mats: float32 [512, 8, 3, 128, 128], P(('space', 'ray')), may hold values from -0.109375 to 0.109375
- neighbours: int32 [512, 8], P(('space', 'ray')), may hold values from 0 to 511, as said below
- self_inverse: float32 [512, 128, 128], P(('space', 'ray')), may hold values from -3 to 4
- radiation: float32 [512, 8192, 128], P(('space', 'ray')), may hold values from -0.1875 to 0.1875
- directions: float32 [3, 8192], replicated, may hold values from -1 to 1, as said below
- centers: float32 [3, 16], replicated, may hold values from -1 to 32, as said below
- counts: int32 [512], P(('space', 'ray')), may hold values from 32 to 128
Outputs:
- currents: float32 [2, 65536], P(None, ('space', 'ray'))
The draws below stay inside these ranges and needn't reach their ends.
Inputs may be any that keep to these rules, and one draw needn't show every extreme that they name: `neighbours`: every neighbour is a box within 4 boxes of its row's box. `directions`: each column is a unit vector. `centers`: the first coordinate of column c lies within 0.4 of 2 c, the others within -1 and 1.
All inputs are finite; a program needn't handle non-finite values.
Results may differ from the reference program's by a relative error of at most 0.0003.
Values sent between devices are 32-bit elements; how exact they have to be, the bound alone decides.
No kernel may reach another device: no remote copies, remote signals or barrier semaphores. Data moves between devices by JAX's collectives and lax.ppermute only.
A program may use at most 128 MiB of HBM per device.

```python
import jax
import jax.numpy as jnp
from jax import lax

PB = 128
BOX_DEV = 4
K = 64
TAU = 48
KN = 3
NB = 8
RAYS = 8192
STEPS = 2
BOXES = 512
PATCHES = 65536
CLUSTERS = 16


def draw_neighbours(key, part):
    box_ids = jnp.arange(BOXES, dtype=jnp.int32)[:, None]
    offsets = jax.random.randint(jax.random.fold_in(key, 11), (BOXES, NB), -BOX_DEV, BOX_DEV + 1, dtype=jnp.int32)
    return jnp.clip(box_ids + offsets, 0, BOXES - 1).astype(jnp.int32)


def draw_self_inverse(key, part):
    noise = jnp.clip(jax.random.normal(jax.random.fold_in(key, 12), (BOXES, PB, PB), jnp.float32), -6.0, 6.0)
    return jnp.eye(PB, dtype=jnp.float32)[None] + 0.5 * noise / jnp.sqrt(float(PB))


def draw_directions(key, part):
    raw = jax.random.normal(jax.random.fold_in(key, 13), (3, RAYS), jnp.float32)
    length = jnp.sqrt(jnp.sum(raw * raw, axis=0, keepdims=True)) + 1e-06
    return raw / length


def draw_centers(key, part):
    first = 2.0 * jnp.arange(CLUSTERS, dtype=jnp.float32) + jax.random.uniform(jax.random.fold_in(key, 14), (CLUSTERS,), jnp.float32, -0.4, 0.4)
    others = jax.random.uniform(jax.random.fold_in(key, 15), (2, CLUSTERS), jnp.float32, -1.0, 1.0)
    return jnp.concatenate([first[None], others], axis=0)


def touch_ends(drawn, rng, smallest, top_value):
    place = [jax.random.randint(jax.random.fold_in(rng, axis), (), 0, length) for axis, length in enumerate(drawn.shape)]
    longest = drawn.shape.index(max(drawn.shape))
    neighbour = place[:longest] + [(place[longest] + 1) % drawn.shape[longest]] + place[longest + 1:]
    return drawn.at[tuple(place)].set(smallest).at[tuple(neighbour)].set(top_value)


def level_of(key, dims, shards, smallest, high):
    gain = 1.0
    for dim, shards_of in shards:
        draws = jax.random.uniform(jax.random.fold_in(jax.random.fold_in(key, 6), dim), (shards_of,), jnp.float32, smallest / len(shards), high / len(shards))
        gain = gain * jnp.repeat(jnp.exp(draws), dims[dim] // shards_of).reshape((-1,) + (1,) * (len(dims) - 1 - dim))
    return gain


def scatter_about(rng, extent, spread, limit, shards=(), kind=jnp.bfloat16):
    result = spread * jax.random.normal(rng, extent, jnp.float32)
    if shards:
        result = result * level_of(rng, extent, shards, -0.22, 0.18)
    return jnp.clip(result, -limit, limit).astype(kind)


def setup_inputs(seed: int = 0) -> dict:
    key_list = jax.random.split(jax.random.key(seed), 10)
    excite = scatter_about(key_list[0], (STEPS, PATCHES), 1.0, 6.0, ((1, 128),), jnp.float32)
    history = scatter_about(key_list[1], (K, PATCHES), 1.0, 6.0, ((1, 128),), jnp.float32)
    near_mats = scatter_about(key_list[2], (BOXES, NB, KN, PB, PB), (PB * NB * KN) ** -0.5, 0.109375, ((0, 128),), jnp.float32)
    neighbours = draw_neighbours(jax.random.fold_in(key_list[9], 71), 0)
    self_inverse = draw_self_inverse(jax.random.fold_in(key_list[9], 71), 0)
    radiation = scatter_about(key_list[5], (BOXES, RAYS, PB), (PB * RAYS // 1024) ** -0.5, 0.1875, ((0, 128),), jnp.float32)
    directions = draw_directions(jax.random.fold_in(key_list[9], 71), 0)
    centers = draw_centers(jax.random.fold_in(key_list[9], 71), 0)
    counts = touch_ends(jax.random.randint(key_list[8], (BOXES,), PB // 4, PB + 1), jax.random.fold_in(key_list[8], 1), PB // 4, PB).astype(jnp.int32)
    return dict(excite=excite, history=history, near_mats=near_mats, neighbours=neighbours, self_inverse=self_inverse, radiation=radiation, directions=directions, centers=centers, counts=counts)


HIGHEST_PRECISION = lax.Precision.HIGHEST

def temporal_basis(levels, length, lag_steps):
    orders = jnp.arange(levels, dtype=jnp.float32)
    return jnp.sqrt(2.0 / length) * jnp.cos(jnp.pi * (orders[:, None] + 0.5) * (lag_steps[None, :] + 0.5) / length)

def pair_lags(unit_dirs, source_centre, target_centre, length, reach):
    separation = target_centre[:, None, :] - source_centre[:, :, None]
    along = jnp.einsum('xd,xab->dab', unit_dirs, separation, precision=HIGHEST_PRECISION)
    return length * 0.125 + length * 0.375 * (1.0 + along / reach)

def pair_gains(unit_dirs, source_centre, target_centre, source_ids, target_ids):
    separation = target_centre[:, None, :] - source_centre[:, :, None]
    distant = jnp.abs(target_ids[None, :] - source_ids[:, None]) >= 2
    distance = jnp.sqrt(lax.optimization_barrier(jnp.sum(separation * separation, axis=0)))
    distance = jnp.where(distant, distance, 1.0)
    cosine = jnp.einsum('xd,xab->dab', unit_dirs, separation, precision=HIGHEST_PRECISION) / distance[None]
    return jnp.where(distant[None], (1.0 + cosine) / (2.0 * distance[None]), 0.0)

def reference(excite, history, near_mats, neighbours, self_inverse, radiation, directions, centers, counts):
    box_total = near_mats.shape[0]
    per_cluster = box_total // CLUSTERS
    reach = 2.0 * CLUSTERS + 4.0
    basis = temporal_basis(TAU, K, jnp.arange(K, dtype=jnp.float32))
    cluster_ids = jnp.arange(CLUSTERS, dtype=jnp.int32)
    radiation_map = radiation.reshape(CLUSTERS, per_cluster, RAYS, PB)
    occupied = jnp.arange(PB, dtype=jnp.int32)[None, :] < counts[:, None]
    results = []
    for instant in range(STEPS):
        recent = history[:KN].reshape(KN, box_total, PB)
        nearby = recent[:, neighbours]
        near_term = jnp.einsum('bjkpq,kbjq->bp', near_mats, nearby, precision=HIGHEST_PRECISION)
        projected = jnp.dot(basis, history, precision=HIGHEST_PRECISION).reshape(TAU, CLUSTERS, per_cluster, PB)
        outgoing = jnp.einsum('cbdp,mcbp->cdm', radiation_map, projected, precision=HIGHEST_PRECISION)
        flipped = jnp.transpose(outgoing, (2, 1, 0))

        def target_sample(target):
            target_centre = lax.dynamic_slice_in_dim(centers, target, 1, 1)
            target_ids = jnp.reshape(target, (1,)).astype(jnp.int32)
            weights = pair_gains(directions, centers, target_centre, cluster_ids, target_ids)[:, :, 0]
            lags = pair_lags(directions, centers, target_centre, K, reach)[:, :, 0]
            evaluate = temporal_basis(TAU, K, lags.reshape(-1)).reshape(TAU, RAYS, CLUSTERS)
            per_pair = lax.optimization_barrier(jnp.sum(flipped * evaluate, axis=0))
            return lax.optimization_barrier(jnp.sum(weights * per_pair, axis=1))
        sampled = lax.map(target_sample, cluster_ids)
        far_term = jnp.einsum('cbdp,cd->cbp', radiation_map, sampled, precision=HIGHEST_PRECISION).reshape(box_total, PB)
        right_side = excite[instant].reshape(box_total, PB) - near_term - far_term
        solved = jnp.einsum('bpq,bq->bp', self_inverse, right_side, precision=HIGHEST_PRECISION)
        solved = jnp.where(occupied, solved, 0.0).reshape(box_total * PB)
        results.append(solved)
        history = jnp.concatenate([solved[None], history[:-1]], axis=0)
    return jnp.stack(results)
```

```python
import functools
import math

import jax
import jax.numpy as jnp
import numpy as np
from jax import lax
from jax.experimental import pallas as pl
from jax.experimental.pallas import tpu as pltpu
from jax.sharding import PartitionSpec as P

PB = 128
K = 64
TAU = 48
KN = 3
STEPS = 2
NB = 8
BOXES_HERE = 4
CLUSTERS = 16
RAYS = 8192
ROWS = RAYS // 128
BLOCK = 1024
STEPS_D = RAYS // BLOCK
REACH = 2.0 * CLUSTERS + 4.0
VMEM = pltpu.VMEM
F32 = jnp.float32
BF16 = jnp.bfloat16


def basis_table():
    m = np.arange(TAU)[:, None] + 0.5
    k = np.arange(K)[None, :] + 0.5
    return np.sqrt(2.0 / K) * np.cos(np.pi * m * k / K)


def projection_table():
    basis = basis_table()
    table = np.zeros((128, K))
    table[:TAU] = basis
    table[TAU : 2 * TAU, : K - 1] = basis[:, 1:]
    return table.astype(np.float32)


def split_two(x):
    high = x.astype(BF16)
    return high, (x - high.astype(F32)).astype(BF16)


def identity_mask():
    return lax.broadcasted_iota(jnp.int32, (128, 128), 0) == lax.broadcasted_iota(
        jnp.int32, (128, 128), 1
    )


def row_of_sums(matrix):
    return jnp.sum(matrix.T, axis=0, keepdims=True)


def translate_kernel(
    space_ref, centers_ref, table_ref, history_ref, dirs_ref, rad_ref,
    first_ref, second_ref, weight_ref, proj_ref, out_ref,
):
    me = space_ref[0]

    @pl.when(pl.program_id(0) == 0)
    def _():
        projected = jnp.dot(
            table_ref[...], history_ref[...], precision=lax.Precision.HIGHEST,
            preferred_element_type=F32,
        )
        for box in range(BOXES_HERE):
            high, low = split_two(projected[:, box * PB : (box + 1) * PB].T)
            rows = pl.ds((box % 2) * PB, PB)
            proj_ref[box // 2, rows, 0:128] = high
            proj_ref[box // 2, rows, 128:256] = low

    highs, lows = [], []
    for box in range(BOXES_HERE):
        high, low = split_two(rad_ref[box])
        highs.append(high)
        lows.append(low)
    total = None
    for pair in range(2):
        high = jnp.concatenate(highs[2 * pair : 2 * pair + 2], axis=1)
        low = jnp.concatenate(lows[2 * pair : 2 * pair + 2], axis=1)
        both = jnp.dot(high, proj_ref[pair], preferred_element_type=F32)
        rest = jnp.dot(low, proj_ref[pair, :, 0:128], preferred_element_type=F32)
        part = both[:, :128] + both[:, 128:] + rest
        total = part if total is None else total + part
    for tile in range(BLOCK // 128):
        turned = total[tile * 128 : (tile + 1) * 128, :].T
        for group in range(2 * TAU // 8):
            out_ref[pl.ds(group * 64 + tile, 8, stride=8), :] = turned[
                group * 8 : (group + 1) * 8, :
            ]

    basis_first = basis_table()[:, 0]
    dx, dy, dz = dirs_ref[0], dirs_ref[1], dirs_ref[2]
    cx, cy, cz = centers_ref[0, me], centers_ref[1, me], centers_ref[2, me]

    def group_of_targets(group, _):
        prepared = []
        for inner in range(4):
            target = group * 4 + inner
            sx = centers_ref[0, target] - cx
            sy = centers_ref[1, target] - cy
            sz = centers_ref[2, target] - cz
            squared = jnp.full((8, 128), sx * sx + sy * sy + sz * sz, F32)
            distant = jnp.abs(target - me) >= 2
            inverse = 1.0 / jnp.sqrt(jnp.where(distant, squared, 1.0))
            along = dx * sx + dy * sy + dz * sz
            u = (math.pi / 128.0) * (0.5 + along * (24.0 / REACH))
            v = u * u
            sin = u * (1 + v * (-1 / 6 + v * (1 / 120 + v * (-1 / 5040 + v * (1 / 362880)))))
            cos = 1 + v * (-1 / 2 + v * (1 / 24 + v * (-1 / 720 + v * (1 / 40320))))
            gain = (1.0 + along * inverse) * inverse * (0.5 * math.sqrt(2.0 / K) / math.sqrt(2.0))
            scale = jnp.where(distant, gain * (cos - sin), 0.0)
            prepared.append((target, -4.0 * sin * cos, scale))
        zero = jnp.zeros((8, 128), F32)
        ones = [[zero, zero, zero] for _ in range(4)]
        twos = [[zero, zero, zero] for _ in range(4)]
        for m in reversed(range(TAU)):
            first = out_ref[m * 8 : (m + 1) * 8, :]
            second = out_ref[(TAU + m) * 8 : (TAU + m + 1) * 8, :]
            terms = (first, second, float(basis_first[m]))
            for inner in range(4):
                twice = prepared[inner][1]
                for part in range(3):
                    new = (terms[part] - twos[inner][part]) + twice * ones[inner][part]
                    twos[inner][part] = ones[inner][part]
                    ones[inner][part] = new
        for inner in range(4):
            target, _, scale = prepared[inner]
            for part, ref in enumerate((first_ref, second_ref, weight_ref)):
                ref[target] = scale * (ones[inner][part] - twos[inner][part])
        return 0

    lax.fori_loop(0, CLUSTERS // 4, group_of_targets, 0)


def translate(space, centers, history, dirs, radiation):
    smem = pl.BlockSpec(memory_space=pltpu.SMEM)
    field = pl.BlockSpec((CLUSTERS, 8, 128), lambda i: (0, i, 0))
    shape = jax.ShapeDtypeStruct((CLUSTERS, ROWS, 128), F32)
    return pl.pallas_call(
        translate_kernel,
        grid=(STEPS_D,),
        in_specs=[
            smem,
            smem,
            pl.BlockSpec((128, K), lambda i: (0, 0)),
            pl.BlockSpec((K, BOXES_HERE * PB), lambda i: (0, 0)),
            pl.BlockSpec((3, 8, 128), lambda i: (0, i, 0)),
            pl.BlockSpec((BOXES_HERE, BLOCK, PB), lambda i: (0, i, 0)),
        ],
        out_specs=[field, field, field],
        out_shape=[shape, shape, shape],
        scratch_shapes=[VMEM((2, 256, 256), BF16), VMEM((2 * TAU * 8, 128), F32)],
        compiler_params=pltpu.CompilerParams(vmem_limit_bytes=32 << 20),
        cost_estimate=pl.CostEstimate(flops=8 << 30, bytes_accessed=20 << 20, transcendentals=0),
        name="translate",
    )(space, centers, jnp.asarray(projection_table()), history, dirs, radiation)


def near_kernel(first_box_ref, nb_ref, lower_ref, own_ref, upper_ref, mats_ref, out_ref, win_ref):
    box = pl.program_id(0)

    @pl.when(box == 0)
    def _():
        for k in range(KN):
            for place, ref in enumerate((lower_ref, own_ref, upper_ref)):
                for inner in range(BOXES_HERE):
                    row = (place * BOXES_HERE + inner) * 8 + k
                    win_ref[row : row + 1, :] = ref[k : k + 1, inner * PB : (inner + 1) * PB]

    first = jnp.zeros((128, 128), F32)
    second = jnp.zeros((128, 128), F32)
    for j in range(NB):
        place = (nb_ref[box, j] - first_box_ref[0] + BOXES_HERE) * 8
        rows = [win_ref[pl.ds(place + k, 1), :] for k in range(KN)]
        for k in range(KN):
            first = first + mats_ref[0, j, k] * rows[k]
            if k:
                second = second + mats_ref[0, j, k] * rows[k - 1]
    out_ref[pl.ds(box, 1), :] = row_of_sums(first)
    out_ref[pl.ds(box + BOXES_HERE, 1), :] = row_of_sums(second)


def near_fields(first_box, neighbours, lower, history, upper, near_mats):
    smem = pl.BlockSpec(memory_space=pltpu.SMEM)
    side = pl.BlockSpec((KN, BOXES_HERE * PB), lambda i: (0, 0))
    return pl.pallas_call(
        near_kernel,
        grid=(BOXES_HERE,),
        in_specs=[
            smem,
            smem,
            side,
            pl.BlockSpec((8, BOXES_HERE * PB), lambda i: (0, 0)),
            side,
            pl.BlockSpec((1, NB, KN, PB, PB), lambda i: (i, 0, 0, 0, 0)),
        ],
        out_specs=pl.BlockSpec((2 * BOXES_HERE, PB), lambda i: (0, 0)),
        out_shape=jax.ShapeDtypeStruct((2 * BOXES_HERE, PB), F32),
        scratch_shapes=[VMEM((3 * BOXES_HERE * 8, PB), F32)],
        compiler_params=pltpu.CompilerParams(vmem_limit_bytes=16 << 20),
        cost_estimate=pl.CostEstimate(flops=1 << 30, bytes_accessed=7 << 20, transcendentals=0),
        name="near_fields",
    )(first_box, neighbours, lower, history, upper, near_mats)


def near_again_kernel(
    first_box_ref, nb_ref, lower_ref, own_ref, upper_ref, before_ref, mats_ref, out_ref, win_ref
):
    box = pl.program_id(0)

    @pl.when(box == 0)
    def _():
        for place, ref in enumerate((lower_ref, own_ref, upper_ref)):
            win_ref[place * BOXES_HERE : (place + 1) * BOXES_HERE, :] = ref[...]

    total = jnp.zeros((128, 128), F32)
    for j in range(NB):
        place = nb_ref[box, j] - first_box_ref[0] + BOXES_HERE
        total = total + mats_ref[0, j, 0] * win_ref[pl.ds(place, 1), :]
    out_ref[pl.ds(box, 1), :] = before_ref[pl.ds(box + BOXES_HERE, 1), :] + row_of_sums(total)


def near_again(first_box, neighbours, lower, own, upper, before, near_mats):
    smem = pl.BlockSpec(memory_space=pltpu.SMEM)
    side = pl.BlockSpec((BOXES_HERE, PB), lambda i: (0, 0))
    return pl.pallas_call(
        near_again_kernel,
        grid=(BOXES_HERE,),
        in_specs=[
            smem,
            smem,
            side,
            side,
            side,
            pl.BlockSpec((2 * BOXES_HERE, PB), lambda i: (0, 0)),
            pl.BlockSpec((1, NB, 1, PB, PB), lambda i: (i, 0, 0, 0, 0)),
        ],
        out_specs=side,
        out_shape=jax.ShapeDtypeStruct((BOXES_HERE, PB), F32),
        scratch_shapes=[VMEM((16, PB), F32)],
        compiler_params=pltpu.CompilerParams(vmem_limit_bytes=16 << 20),
        cost_estimate=pl.CostEstimate(flops=1 << 29, bytes_accessed=3 << 20, transcendentals=0),
        name="near_again",
    )(first_box, neighbours, lower, own, upper, before, near_mats)


def far_of_block(samp_ref, rows, rad, sums, ones):
    eye = identity_mask()
    for tile in range(BLOCK // 128):
        row = samp_ref[pl.ds(rows + tile, 1), :]
        high = row.astype(BF16).astype(F32)
        low = row - high
        spread = jnp.concatenate(
            [jnp.where(eye, high, 0.0).astype(BF16), jnp.where(eye, low, 0.0).astype(BF16)], axis=1
        )
        copies = jnp.dot(spread, ones, preferred_element_type=F32)
        for box in range(BOXES_HERE):
            product = rad(box, tile) * copies
            sums[box] = sums[box] + jnp.sum(product.reshape(16, 8, 128), axis=0)
    return sums


def solve(counts_ref, inverse_ref, right_side, box):
    solved = row_of_sums(inverse_ref[box] * right_side)
    live = lax.broadcasted_iota(jnp.int32, (1, PB), 1) < counts_ref[box]
    return jnp.where(live, solved, 0.0)


def first_step_kernel(
    counts_ref, parts_ref, near_ref, excite_ref, inverse_ref, second_ref, weight_ref, rad_hbm,
    current_ref, field_ref, rad_ref, samp_ref, dot_ref, sems,
):
    copies = [
        pltpu.make_async_copy(
            rad_hbm.at[:, pl.ds(i * BLOCK, BLOCK), :],
            rad_ref.at[:, pl.ds(i * BLOCK, BLOCK), :],
            sems.at[i],
        )
        for i in range(STEPS_D)
    ]
    for copy in copies:
        copy.start()
    samp_ref[...] = jnp.sum(parts_ref[...], axis=0)
    ones = jnp.ones((256, 128), BF16)
    sums = [jnp.zeros((8, 128), F32) for _ in range(BOXES_HERE)]
    for i in range(STEPS_D):
        copies[i].wait()
        rad = lambda box, tile, i=i: rad_ref[
            box, i * BLOCK + tile * 128 : i * BLOCK + (tile + 1) * 128, :
        ]
        sums = far_of_block(samp_ref, i * 8, rad, sums, ones)
    currents = []
    for box in range(BOXES_HERE):
        far = jnp.sum(sums[box], axis=0, keepdims=True)
        right_side = (
            excite_ref[0:1, box * PB : (box + 1) * PB] - near_ref[box : box + 1, :] - far
        )
        current = solve(counts_ref, inverse_ref, right_side, box)
        current_ref[box : box + 1, :] = current
        currents.append(current)
    eye = identity_mask()

    def one_block(i, _):
        for tile in range(BLOCK // 128):
            start = pl.multiple_of(i * BLOCK + tile * 128, 128)
            product = rad_ref[0, pl.ds(start, 128), :] * currents[0]
            for box in range(1, BOXES_HERE):
                product = product + rad_ref[box, pl.ds(start, 128), :] * currents[box]
            high, low = split_two(product)
            copies_of = jnp.dot(
                jnp.concatenate([high, low], axis=1), ones, preferred_element_type=F32
            )
            dot_ref[tile : tile + 1, :] = jnp.sum(
                jnp.where(eye, copies_of, 0.0), axis=0, keepdims=True
            )
        response = dot_ref[...]
        rows = pl.ds(pl.multiple_of(i * 8, 8), 8)
        for target in range(CLUSTERS):
            field_ref[target, rows, :] = (
                second_ref[target, rows, :] + weight_ref[target, rows, :] * response
            )
        return 0

    lax.fori_loop(0, STEPS_D, one_block, 0)


def first_step(counts, parts, near, excite, self_inverse, second, weight, radiation):
    smem = pl.BlockSpec(memory_space=pltpu.SMEM)
    vmem = pl.BlockSpec(memory_space=VMEM)
    return pl.pallas_call(
        first_step_kernel,
        in_specs=[smem, vmem, vmem, vmem, vmem, vmem, vmem, pl.BlockSpec(memory_space=pl.ANY)],
        out_specs=[vmem, vmem],
        out_shape=[
            jax.ShapeDtypeStruct((BOXES_HERE, PB), F32),
            jax.ShapeDtypeStruct((CLUSTERS, ROWS, 128), F32),
        ],
        scratch_shapes=[
            VMEM((BOXES_HERE, RAYS, PB), F32),
            VMEM((ROWS, 128), F32),
            VMEM((8, 128), F32),
            pltpu.SemaphoreType.DMA((STEPS_D,)),
        ],
        compiler_params=pltpu.CompilerParams(vmem_limit_bytes=40 << 20),
        cost_estimate=pl.CostEstimate(flops=4 << 30, bytes_accessed=20 << 20, transcendentals=0),
        name="first_step",
    )(counts, parts, near, excite, self_inverse, second, weight, radiation)


def second_step_kernel(
    counts_ref, parts_ref, near_ref, excite_ref, inverse_ref, before_ref, rad_ref,
    out_ref, samp_ref, sum_ref,
):
    i = pl.program_id(0)

    @pl.when(i == 0)
    def _():
        samp_ref[...] = jnp.sum(parts_ref[...], axis=0)
        sum_ref[...] = jnp.zeros_like(sum_ref)

    ones = jnp.ones((256, 128), BF16)
    rad = lambda box, tile: rad_ref[box, tile * 128 : (tile + 1) * 128, :]
    sums = [sum_ref[box] for box in range(BOXES_HERE)]
    sums = far_of_block(samp_ref, i * 8, rad, sums, ones)
    for box in range(BOXES_HERE):
        sum_ref[box] = sums[box]

    @pl.when(i == STEPS_D - 1)
    def _():
        for box in range(BOXES_HERE):
            lanes = slice(box * PB, (box + 1) * PB)
            far = jnp.sum(sum_ref[box], axis=0, keepdims=True)
            right_side = excite_ref[1:2, lanes] - near_ref[box : box + 1, :] - far
            out_ref[0:1, lanes] = before_ref[box : box + 1, :]
            out_ref[1:2, lanes] = solve(counts_ref, inverse_ref, right_side, box)


def second_step(counts, parts, near, excite, self_inverse, before, radiation):
    smem = pl.BlockSpec(memory_space=pltpu.SMEM)
    whole = lambda *shape: pl.BlockSpec(shape, lambda i: (0,) * len(shape))
    return pl.pallas_call(
        second_step_kernel,
        grid=(STEPS_D,),
        in_specs=[
            smem,
            whole(8, ROWS, 128),
            whole(BOXES_HERE, PB),
            whole(STEPS, BOXES_HERE * PB),
            whole(BOXES_HERE, PB, PB),
            whole(BOXES_HERE, PB),
            pl.BlockSpec((BOXES_HERE, BLOCK, PB), lambda i: (0, i, 0)),
        ],
        out_specs=whole(STEPS, BOXES_HERE * PB),
        out_shape=jax.ShapeDtypeStruct((STEPS, BOXES_HERE * PB), F32),
        scratch_shapes=[VMEM((ROWS, 128), F32), VMEM((BOXES_HERE, 8, 128), F32)],
        compiler_params=pltpu.CompilerParams(vmem_limit_bytes=32 << 20),
        cost_estimate=pl.CostEstimate(flops=4 << 30, bytes_accessed=20 << 20, transcendentals=0),
        name="second_step",
    )(counts, parts, near, excite, self_inverse, before, radiation)


def from_behind(array, by):
    axis = ("space", "ray")
    size = lax.axis_size(axis)
    pairs = [(i, i + by) for i in range(size) if 0 <= i + by < size]
    return lax.ppermute(array, axis, pairs)


def gathered(field):
    arrived = lax.all_to_all(field, "space", split_axis=0, concat_axis=0, tiled=True)
    mine = jnp.sum(arrived, axis=0)
    size = lax.axis_size("ray")
    copies = jnp.broadcast_to(mine[None], (size, *mine.shape))
    return lax.all_to_all(copies, "ray", split_axis=0, concat_axis=0, tiled=True)


def local(
    excite, history, near_mats, neighbours, self_inverse, radiation, directions, centers, counts
):
    space = lax.axis_index("space").astype(jnp.int32).reshape(1)
    first_box = (lax.axis_index(("space", "ray")) * BOXES_HERE).astype(jnp.int32).reshape(1)
    dirs = directions.reshape(3, ROWS, 128)
    recent = history[:KN]
    lower, upper = from_behind(recent, 1), from_behind(recent, -1)
    first, second, weight = translate(space, centers, history, dirs, radiation)
    parts = gathered(first)
    near = near_fields(first_box, neighbours, lower, history, upper, near_mats)
    current, field = first_step(
        counts, parts, near, excite, self_inverse, second, weight, radiation
    )
    lower, upper = from_behind(current, 1), from_behind(current, -1)
    parts = gathered(field)
    near = near_again(first_box, neighbours, lower, current, upper, near, near_mats)
    return second_step(counts, parts, near, excite, self_inverse, current, radiation)


def solution(mesh):
    placed = (
        P(None, ("space", "ray")),
        P(None, ("space", "ray")),
        P(("space", "ray"), None, None, None, None),
        P(("space", "ray"), None),
        P(("space", "ray"), None, None),
        P(("space", "ray"), None, None),
        P(),
        P(),
        P(("space", "ray")),
    )
    return jax.shard_map(
        local, mesh=mesh, in_specs=placed, out_specs=P(None, ("space", "ray")), check_vma=False
    )
```

```python
import functools
import math

import jax
import jax.numpy as jnp
import numpy as np
from jax import lax
from jax.experimental import pallas as pl
from jax.experimental.pallas import tpu as pltpu
from jax.sharding import PartitionSpec as P

PB = 128
K = 64
TAU = 48
KN = 3
STEPS = 2
NB = 8
BOXES_HERE = 4
CLUSTERS = 16
RAYS = 8192
ROWS = RAYS // 128
BLOCK = 1024
STEPS_D = RAYS // BLOCK
REACH = 2.0 * CLUSTERS + 4.0
VMEM = pltpu.VMEM
F32 = jnp.float32
BF16 = jnp.bfloat16


def basis_table():
    m = np.arange(TAU)[:, None] + 0.5
    k = np.arange(K)[None, :] + 0.5
    return np.sqrt(2.0 / K) * np.cos(np.pi * m * k / K)


def projection_table():
    basis = basis_table()
    table = np.zeros((128, K))
    table[:TAU] = basis
    table[TAU : 2 * TAU, : K - 1] = basis[:, 1:]
    return table.astype(np.float32)


def split_two(x):
    high = x.astype(BF16)
    return high, (x - high.astype(F32)).astype(BF16)


def identity_mask():
    return lax.broadcasted_iota(jnp.int32, (128, 128), 0) == lax.broadcasted_iota(
        jnp.int32, (128, 128), 1
    )


def row_of_sums(matrix):
    return jnp.sum(matrix.T, axis=0, keepdims=True)


def targets_of(me, centers_ref, dirs, target):
    dx, dy, dz = dirs
    sx = centers_ref[0, target] - centers_ref[0, me]
    sy = centers_ref[1, target] - centers_ref[1, me]
    sz = centers_ref[2, target] - centers_ref[2, me]
    squared = jnp.full((8, 128), sx * sx + sy * sy + sz * sz, F32)
    distant = jnp.abs(target - me) >= 2
    inverse = 1.0 / jnp.sqrt(jnp.where(distant, squared, 1.0))
    along = dx * sx + dy * sy + dz * sz
    u = (math.pi / 128.0) * (0.5 + along * (24.0 / REACH))
    v = u * u
    sin = u * (1 + v * (-1 / 6 + v * (1 / 120 + v * (-1 / 5040 + v * (1 / 362880)))))
    cos = 1 + v * (-1 / 2 + v * (1 / 24 + v * (-1 / 720 + v * (1 / 40320))))
    gain = (1.0 + along * inverse) * inverse * (0.5 * math.sqrt(2.0 / K) / math.sqrt(2.0))
    return -4.0 * sin * cos, jnp.where(distant, gain * (cos - sin), 0.0)


def clenshaw(terms_of, prepared, parts):
    zero = jnp.zeros((8, 128), F32)
    ones = [[zero] * parts for _ in prepared]
    twos = [[zero] * parts for _ in prepared]
    for m in reversed(range(TAU)):
        terms = terms_of(m)
        for inner, (twice, _) in enumerate(prepared):
            for part in range(parts):
                new = (terms[part] - twos[inner][part]) + twice * ones[inner][part]
                twos[inner][part] = ones[inner][part]
                ones[inner][part] = new
    return [
        [scale * (one - two) for one, two in zip(ones[inner], twos[inner])]
        for inner, (_, scale) in enumerate(prepared)
    ]


def translate_kernel(
    space_ref, centers_ref, table_hbm, history_hbm, dirs_hbm, rad_hbm,
    first_ref, second_ref, lines_ref,
    rad_ref, table_ref, history_ref, dirs_ref, proj_ref, out_ref, small_sems, sems,
):
    me = space_ref[0]
    small = [
        pltpu.make_async_copy(source, target, small_sems.at[i])
        for i, (source, target) in enumerate(
            ((table_hbm, table_ref), (history_hbm, history_ref), (dirs_hbm, dirs_ref))
        )
    ]
    copies = [
        pltpu.make_async_copy(
            rad_hbm.at[:, pl.ds(i * BLOCK, BLOCK), :],
            rad_ref.at[:, pl.ds(i * BLOCK, BLOCK), :],
            sems.at[i],
        )
        for i in range(STEPS_D)
    ]
    for copy in small + copies:
        copy.start()
    for copy in small:
        copy.wait()
    for axis in range(3):
        for row in range(ROWS):
            lines_ref[axis * ROWS + row : axis * ROWS + row + 1, :] = dirs_ref[
                axis : axis + 1, row * 128 : (row + 1) * 128
            ]
    projected = jnp.dot(
        table_ref[...], history_ref[...], precision=lax.Precision.HIGHEST,
        preferred_element_type=F32,
    )
    for box in range(BOXES_HERE):
        high, low = split_two(projected[:, box * PB : (box + 1) * PB].T)
        rows = pl.ds((box % 2) * PB, PB)
        proj_ref[box // 2, rows, 0:128] = high
        proj_ref[box // 2, rows, 128:256] = low

    def project(i):
        highs, lows = [], []
        for box in range(BOXES_HERE):
            high, low = split_two(rad_ref[box, i * BLOCK : (i + 1) * BLOCK, :])
            highs.append(high)
            lows.append(low)
        total = None
        for pair in range(2):
            high = jnp.concatenate(highs[2 * pair : 2 * pair + 2], axis=1)
            low = jnp.concatenate(lows[2 * pair : 2 * pair + 2], axis=1)
            both = jnp.dot(high, proj_ref[pair], preferred_element_type=F32)
            rest = jnp.dot(low, proj_ref[pair, :, 0:128], preferred_element_type=F32)
            part = both[:, :128] + both[:, 128:] + rest
            total = part if total is None else total + part
        for tile in range(BLOCK // 128):
            turned = total[tile * 128 : (tile + 1) * 128, :].T
            row = i * 8 + tile
            for group in range(TAU // 8):
                place = pl.ds(group * 8 * ROWS + row, 8, stride=ROWS)
                out_ref[place, :] = turned[group * 8 : (group + 1) * 8, :]
                second_ref[place, :] = turned[TAU + group * 8 : TAU + (group + 1) * 8, :]

    def spread(i):
        rows = slice(i * 8, (i + 1) * 8)
        dirs = [lines_ref[axis * ROWS + i * 8 : axis * ROWS + (i + 1) * 8, :] for axis in range(3)]
        terms_of = lambda m: (out_ref[m * ROWS + i * 8 : m * ROWS + (i + 1) * 8, :],)
        for group in range(CLUSTERS // 8):
            targets = range(group * 8, (group + 1) * 8)
            prepared = [targets_of(me, centers_ref, dirs, target) for target in targets]
            for target, result in zip(targets, clenshaw(terms_of, prepared, 1)):
                first_ref[target, rows, :] = result[0]

    for i in range(STEPS_D):
        copies[i].wait()
        project(i)
        if i:
            spread(i - 1)
    spread(STEPS_D - 1)


def in_hbm(x):
    return pltpu.with_memory_space_constraint(x, pltpu.HBM)


def translate(space, centers, history, dirs, radiation):
    smem = pl.BlockSpec(memory_space=pltpu.SMEM)
    hbm = pl.BlockSpec(memory_space=pltpu.HBM)
    vmem = pl.BlockSpec(memory_space=VMEM)
    table = jnp.asarray(projection_table())
    return pl.pallas_call(
        translate_kernel,
        in_specs=[smem, smem, hbm, hbm, hbm, hbm],
        out_specs=[vmem, vmem, vmem],
        out_shape=[
            jax.ShapeDtypeStruct((CLUSTERS, ROWS, 128), F32),
            jax.ShapeDtypeStruct((TAU * ROWS, 128), F32),
            jax.ShapeDtypeStruct((3 * ROWS, 128), F32),
        ],
        scratch_shapes=[
            VMEM(radiation.shape, F32),
            VMEM((128, K), F32),
            VMEM(history.shape, F32),
            VMEM(dirs.shape, F32),
            VMEM((2, 256, 256), BF16),
            VMEM((TAU * ROWS, 128), F32),
            pltpu.SemaphoreType.DMA((3,)),
            pltpu.SemaphoreType.DMA((STEPS_D,)),
        ],
        compiler_params=pltpu.CompilerParams(vmem_limit_bytes=28 << 20),
        cost_estimate=pl.CostEstimate(flops=8 << 30, bytes_accessed=20 << 20, transcendentals=0),
        name="translate",
    )(space, in_hbm(centers), in_hbm(table), in_hbm(history), in_hbm(dirs), in_hbm(radiation))


def known_kernel(space_ref, centers_ref, out_ref, lines_ref, second_ref, weight_ref):
    me = space_ref[0]
    basis_first = basis_table()[:, 0]

    def block(i, _):
        rows = pl.ds(pl.multiple_of(i * 8, 8), 8)
        dirs = [
            lines_ref[pl.ds(pl.multiple_of(axis * ROWS + i * 8, 8), 8), :] for axis in range(3)
        ]
        terms_of = lambda m: (
            out_ref[pl.ds(pl.multiple_of(m * ROWS + i * 8, 8), 8), :],
            float(basis_first[m]),
        )
        for group in range(CLUSTERS // 4):
            targets = range(group * 4, (group + 1) * 4)
            prepared = [targets_of(me, centers_ref, dirs, target) for target in targets]
            for target, result in zip(targets, clenshaw(terms_of, prepared, 2)):
                second_ref[target, rows, :] = result[0]
                weight_ref[target, rows, :] = result[1]
        return 0

    lax.fori_loop(0, STEPS_D, block, 0)


def known_part(space, centers, out, lines):
    smem = pl.BlockSpec(memory_space=pltpu.SMEM)
    vmem = pl.BlockSpec(memory_space=VMEM)
    shape = jax.ShapeDtypeStruct((CLUSTERS, ROWS, 128), F32)
    return pl.pallas_call(
        known_kernel,
        in_specs=[smem, smem, vmem, vmem],
        out_specs=[vmem, vmem],
        out_shape=[shape, shape],
        compiler_params=pltpu.CompilerParams(vmem_limit_bytes=8 << 20),
        cost_estimate=pl.CostEstimate(flops=20 << 20, bytes_accessed=4 << 20, transcendentals=0),
        name="known_part",
    )(space, centers, out, lines)


def near_kernel(first_box_ref, nb_ref, lower_ref, own_ref, upper_ref, mats_ref, out_ref, win_ref):
    box = pl.program_id(0)

    @pl.when(box == 0)
    def _():
        for k in range(KN):
            for place, ref in enumerate((lower_ref, own_ref, upper_ref)):
                for inner in range(BOXES_HERE):
                    row = (place * BOXES_HERE + inner) * 8 + k
                    win_ref[row : row + 1, :] = ref[k : k + 1, inner * PB : (inner + 1) * PB]

    first = jnp.zeros((128, 128), F32)
    second = jnp.zeros((128, 128), F32)
    for j in range(NB):
        place = (nb_ref[box, j] - first_box_ref[0] + BOXES_HERE) * 8
        rows = [win_ref[pl.ds(place + k, 1), :] for k in range(KN)]
        for k in range(KN):
            first = first + mats_ref[0, j, k] * rows[k]
            if k:
                second = second + mats_ref[0, j, k] * rows[k - 1]
    out_ref[pl.ds(box, 1), :] = row_of_sums(first)
    out_ref[pl.ds(box + BOXES_HERE, 1), :] = row_of_sums(second)


def near_fields(first_box, neighbours, lower, history, upper, near_mats):
    smem = pl.BlockSpec(memory_space=pltpu.SMEM)
    side = pl.BlockSpec((KN, BOXES_HERE * PB), lambda i: (0, 0))
    return pl.pallas_call(
        near_kernel,
        grid=(BOXES_HERE,),
        in_specs=[
            smem,
            smem,
            side,
            pl.BlockSpec((8, BOXES_HERE * PB), lambda i: (0, 0)),
            side,
            pl.BlockSpec((1, NB, KN, PB, PB), lambda i: (i, 0, 0, 0, 0)),
        ],
        out_specs=pl.BlockSpec((2 * BOXES_HERE, PB), lambda i: (0, 0)),
        out_shape=jax.ShapeDtypeStruct((2 * BOXES_HERE, PB), F32),
        scratch_shapes=[VMEM((3 * BOXES_HERE * 8, PB), F32)],
        compiler_params=pltpu.CompilerParams(vmem_limit_bytes=6 << 20),
        cost_estimate=pl.CostEstimate(flops=1 << 30, bytes_accessed=7 << 20, transcendentals=0),
        name="near_fields",
    )(first_box, neighbours, lower, history, upper, near_mats)


def near_again_kernel(
    first_box_ref, nb_ref, lower_ref, own_ref, upper_ref, before_ref, mats_ref, out_ref, win_ref
):
    box = pl.program_id(0)

    @pl.when(box == 0)
    def _():
        for place, ref in enumerate((lower_ref, own_ref, upper_ref)):
            win_ref[place * BOXES_HERE : (place + 1) * BOXES_HERE, :] = ref[...]

    total = jnp.zeros((128, 128), F32)
    for j in range(NB):
        place = nb_ref[box, j] - first_box_ref[0] + BOXES_HERE
        total = total + mats_ref[0, j, 0] * win_ref[pl.ds(place, 1), :]
    out_ref[pl.ds(box, 1), :] = before_ref[pl.ds(box + BOXES_HERE, 1), :] + row_of_sums(total)


def near_again(first_box, neighbours, lower, own, upper, before, near_mats):
    smem = pl.BlockSpec(memory_space=pltpu.SMEM)
    side = pl.BlockSpec((BOXES_HERE, PB), lambda i: (0, 0))
    return pl.pallas_call(
        near_again_kernel,
        grid=(BOXES_HERE,),
        in_specs=[
            smem,
            smem,
            side,
            side,
            side,
            pl.BlockSpec((2 * BOXES_HERE, PB), lambda i: (0, 0)),
            pl.BlockSpec((1, NB, 1, PB, PB), lambda i: (i, 0, 0, 0, 0)),
        ],
        out_specs=side,
        out_shape=jax.ShapeDtypeStruct((BOXES_HERE, PB), F32),
        scratch_shapes=[VMEM((16, PB), F32)],
        compiler_params=pltpu.CompilerParams(vmem_limit_bytes=6 << 20),
        cost_estimate=pl.CostEstimate(flops=1 << 29, bytes_accessed=3 << 20, transcendentals=0),
        name="near_again",
    )(first_box, neighbours, lower, own, upper, before, near_mats)


def far_of_block(samp_ref, rows, rad, sums, ones):
    eye = identity_mask()
    for tile in range(BLOCK // 128):
        row = samp_ref[pl.ds(rows + tile, 1), :]
        high = row.astype(BF16).astype(F32)
        low = row - high
        spread = jnp.concatenate(
            [jnp.where(eye, high, 0.0).astype(BF16), jnp.where(eye, low, 0.0).astype(BF16)], axis=1
        )
        copies = jnp.dot(spread, ones, preferred_element_type=F32)
        for box in range(BOXES_HERE):
            product = rad(box, tile) * copies
            sums[box] = sums[box] + jnp.sum(product.reshape(16, 8, 128), axis=0)
    return sums


def solve(counts_ref, inverse_ref, right_side, box):
    solved = row_of_sums(inverse_ref[box] * right_side)
    live = lax.broadcasted_iota(jnp.int32, (1, PB), 1) < counts_ref[box]
    return jnp.where(live, solved, 0.0)


def far_of_all(samp_ref, parts_ref, rad_hbm, rad_ref, sems):
    copies = [
        pltpu.make_async_copy(
            rad_hbm.at[:, pl.ds(i * BLOCK, BLOCK), :],
            rad_ref.at[:, pl.ds(i * BLOCK, BLOCK), :],
            sems.at[i],
        )
        for i in range(STEPS_D)
    ]
    for copy in copies:
        copy.start()
    samp_ref[...] = jnp.sum(parts_ref[...], axis=0)
    ones = jnp.ones((256, 128), BF16)
    sums = [jnp.zeros((8, 128), F32) for _ in range(BOXES_HERE)]
    for i in range(STEPS_D):
        copies[i].wait()
        rad = lambda box, tile, i=i: rad_ref[
            box, i * BLOCK + tile * 128 : i * BLOCK + (tile + 1) * 128, :
        ]
        sums = far_of_block(samp_ref, i * 8, rad, sums, ones)
    return sums


def first_step_kernel(
    counts_ref, parts_ref, near_ref, excite_ref, inverse_ref, second_ref, weight_ref, rad_hbm,
    current_ref, field_ref, rad_ref, samp_ref, dot_ref, sems,
):
    sums = far_of_all(samp_ref, parts_ref, rad_hbm, rad_ref, sems)
    ones = jnp.ones((256, 128), BF16)
    currents = []
    for box in range(BOXES_HERE):
        far = jnp.sum(sums[box], axis=0, keepdims=True)
        right_side = (
            excite_ref[0:1, box * PB : (box + 1) * PB] - near_ref[box : box + 1, :] - far
        )
        current = solve(counts_ref, inverse_ref, right_side, box)
        current_ref[box : box + 1, :] = current
        currents.append(current)
    eye = identity_mask()

    def one_block(i, _):
        for tile in range(BLOCK // 128):
            start = pl.multiple_of(i * BLOCK + tile * 128, 128)
            product = rad_ref[0, pl.ds(start, 128), :] * currents[0]
            for box in range(1, BOXES_HERE):
                product = product + rad_ref[box, pl.ds(start, 128), :] * currents[box]
            high, low = split_two(product)
            copies_of = jnp.dot(
                jnp.concatenate([high, low], axis=1), ones, preferred_element_type=F32
            )
            dot_ref[tile : tile + 1, :] = jnp.sum(
                jnp.where(eye, copies_of, 0.0), axis=0, keepdims=True
            )
        response = dot_ref[...]
        rows = pl.ds(pl.multiple_of(i * 8, 8), 8)
        for target in range(CLUSTERS):
            field_ref[target, rows, :] = (
                second_ref[target, rows, :] + weight_ref[target, rows, :] * response
            )
        return 0

    lax.fori_loop(0, STEPS_D, one_block, 0)


def first_step(counts, parts, near, excite, self_inverse, second, weight, radiation):
    smem = pl.BlockSpec(memory_space=pltpu.SMEM)
    vmem = pl.BlockSpec(memory_space=VMEM)
    return pl.pallas_call(
        first_step_kernel,
        in_specs=[smem] + [vmem] * 6 + [pl.BlockSpec(memory_space=pltpu.HBM)],
        out_specs=[vmem, vmem],
        out_shape=[
            jax.ShapeDtypeStruct((BOXES_HERE, PB), F32),
            jax.ShapeDtypeStruct((CLUSTERS, ROWS, 128), F32),
        ],
        scratch_shapes=[
            VMEM(radiation.shape, F32),
            VMEM((ROWS, 128), F32),
            VMEM((8, 128), F32),
            pltpu.SemaphoreType.DMA((STEPS_D,)),
        ],
        compiler_params=pltpu.CompilerParams(vmem_limit_bytes=28 << 20),
        cost_estimate=pl.CostEstimate(flops=4 << 30, bytes_accessed=20 << 20, transcendentals=0),
        name="first_step",
    )(counts, parts, near, excite, self_inverse, second, weight, in_hbm(radiation))


def second_step_kernel(
    counts_ref, parts_ref, near_ref, excite_ref, inverse_ref, before_ref, rad_hbm,
    out_ref, rad_ref, samp_ref, sems,
):
    sums = far_of_all(samp_ref, parts_ref, rad_hbm, rad_ref, sems)
    for box in range(BOXES_HERE):
        lanes = slice(box * PB, (box + 1) * PB)
        far = jnp.sum(sums[box], axis=0, keepdims=True)
        right_side = excite_ref[1:2, lanes] - near_ref[box : box + 1, :] - far
        out_ref[0:1, lanes] = before_ref[box : box + 1, :]
        out_ref[1:2, lanes] = solve(counts_ref, inverse_ref, right_side, box)


def second_step(counts, parts, near, excite, self_inverse, before, radiation):
    smem = pl.BlockSpec(memory_space=pltpu.SMEM)
    vmem = pl.BlockSpec(memory_space=VMEM)
    return pl.pallas_call(
        second_step_kernel,
        in_specs=[smem] + [vmem] * 5 + [pl.BlockSpec(memory_space=pltpu.HBM)],
        out_specs=vmem,
        out_shape=jax.ShapeDtypeStruct((STEPS, BOXES_HERE * PB), F32),
        scratch_shapes=[
            VMEM(radiation.shape, F32),
            VMEM((ROWS, 128), F32),
            pltpu.SemaphoreType.DMA((STEPS_D,)),
        ],
        compiler_params=pltpu.CompilerParams(vmem_limit_bytes=28 << 20),
        cost_estimate=pl.CostEstimate(flops=4 << 30, bytes_accessed=20 << 20, transcendentals=0),
        name="second_step",
    )(counts, parts, near, excite, self_inverse, before, in_hbm(radiation))


def from_behind(array, by):
    axis = ("space", "ray")
    size = lax.axis_size(axis)
    pairs = [(i, i + by) for i in range(size) if 0 <= i + by < size]
    return lax.ppermute(array, axis, pairs)


def sum_kernel(arrived_ref, copies_ref):
    total = jnp.sum(arrived_ref[...], axis=0)
    for copy in range(copies_ref.shape[0]):
        copies_ref[copy] = total


def summed_copies(arrived, copies):
    vmem = pl.BlockSpec(memory_space=VMEM)
    return pl.pallas_call(
        sum_kernel,
        in_specs=[vmem],
        out_specs=vmem,
        out_shape=jax.ShapeDtypeStruct((copies, *arrived.shape[1:]), F32),
        compiler_params=pltpu.CompilerParams(vmem_limit_bytes=4 << 20),
        cost_estimate=pl.CostEstimate(flops=1 << 17, bytes_accessed=1 << 20, transcendentals=0),
        name="summed_copies",
    )(arrived)


def gathered(field, beside):
    arrived = lax.all_to_all(field, "space", split_axis=0, concat_axis=0, tiled=True)
    copies = summed_copies(arrived, lax.axis_size("ray"))
    copies, beside = lax.optimization_barrier((copies, beside))
    return lax.all_to_all(copies, "ray", split_axis=0, concat_axis=0, tiled=True), beside


def local(
    excite, history, near_mats, neighbours, self_inverse, radiation, directions, centers, counts
):
    space = lax.axis_index("space").astype(jnp.int32).reshape(1)
    first_box = (lax.axis_index(("space", "ray")) * BOXES_HERE).astype(jnp.int32).reshape(1)
    recent = history[:KN]
    first, out, lines = translate(space, centers, history, directions, radiation)
    lower, upper = from_behind(recent, 1), from_behind(recent, -1)
    second, weight = known_part(space, centers, out, lines)
    parts, (lower, upper, second, weight) = gathered(first, (lower, upper, second, weight))
    near = near_fields(first_box, neighbours, lower, history, upper, near_mats)
    current, field = first_step(counts, parts, near, excite, self_inverse, second, weight, radiation)
    lower, upper = from_behind(current, 1), from_behind(current, -1)
    parts, (lower, upper) = gathered(field, (lower, upper))
    near = near_again(first_box, neighbours, lower, current, upper, near, near_mats)
    return second_step(counts, parts, near, excite, self_inverse, current, radiation)


def solution(mesh):
    placed = (
        P(None, ("space", "ray")),
        P(None, ("space", "ray")),
        P(("space", "ray"), None, None, None, None),
        P(("space", "ray"), None),
        P(("space", "ray"), None, None),
        P(("space", "ray"), None, None),
        P(),
        P(),
        P(("space", "ray")),
    )
    return jax.shard_map(
        local, mesh=mesh, in_specs=placed, out_specs=P(None, ("space", "ray")), check_vma=False
    )
```

```python
import functools
import math

import jax
import jax.numpy as jnp
import numpy as np
from jax import lax
from jax.experimental import pallas as pl
from jax.experimental.pallas import tpu as pltpu
from jax.sharding import PartitionSpec as P

PB = 128
K = 64
TAU = 48
KN = 3
STEPS = 2
NB = 8
BOXES_HERE = 4
CLUSTERS = 16
FAR_TARGETS = 14
RAYS = 8192
ROWS = RAYS // 128
LINE = ROWS + 8
BLOCK = 1024
STEPS_D = RAYS // BLOCK
AHEAD = 2
AHEAD_FAR = 4
REACH = 2.0 * CLUSTERS + 4.0
VMEM = pltpu.VMEM
F32 = jnp.float32
BF16 = jnp.bfloat16


def basis_table():
    m = np.arange(TAU)[:, None] + 0.5
    k = np.arange(K)[None, :] + 0.5
    return np.sqrt(2.0 / K) * np.cos(np.pi * m * k / K)


def projection_table():
    basis = basis_table()
    table = np.zeros((128, K))
    table[:TAU] = basis
    table[TAU : 2 * TAU, : K - 1] = basis[:, 1:]
    return table.astype(np.float32)


def split_two(x):
    high = x.astype(BF16)
    return high, (x - high.astype(F32)).astype(BF16)


def identity_mask():
    return lax.broadcasted_iota(jnp.int32, (128, 128), 0) == lax.broadcasted_iota(
        jnp.int32, (128, 128), 1
    )


def row_of_sums(matrix):
    return jnp.sum(matrix.T, axis=0, keepdims=True)


def targets_of(me, centers_ref, dirs, target):
    dx, dy, dz = dirs
    sx = centers_ref[0, target] - centers_ref[0, me]
    sy = centers_ref[1, target] - centers_ref[1, me]
    sz = centers_ref[2, target] - centers_ref[2, me]
    squared = jnp.full((8, 128), sx * sx + sy * sy + sz * sz, F32)
    distant = jnp.abs(target - me) >= 2
    inverse = 1.0 / jnp.sqrt(jnp.where(distant, squared, 1.0))
    along = dx * sx + dy * sy + dz * sz
    u = (math.pi / 128.0) * (0.5 + along * (24.0 / REACH))
    v = u * u
    sin = u * (1 + v * (-1 / 6 + v * (1 / 120 + v * (-1 / 5040 + v * (1 / 362880)))))
    cos = 1 + v * (-1 / 2 + v * (1 / 24 + v * (-1 / 720 + v * (1 / 40320))))
    gain = (1.0 + along * inverse) * inverse * (0.5 * math.sqrt(2.0 / K) / math.sqrt(2.0))
    return -4.0 * sin * cos, jnp.where(distant, gain * (cos - sin), 0.0)


def clenshaw(terms_of, prepared, parts):
    zero = jnp.zeros((8, 128), F32)
    ones = [[zero] * parts for _ in prepared]
    twos = [[zero] * parts for _ in prepared]
    for m in reversed(range(TAU)):
        terms = terms_of(m)
        for inner, (twice, _) in enumerate(prepared):
            for part in range(parts):
                new = (terms[part] - twos[inner][part]) + twice * ones[inner][part]
                twos[inner][part] = ones[inner][part]
                ones[inner][part] = new
    return [
        [scale * (one - two) for one, two in zip(ones[inner], twos[inner])]
        for inner, (_, scale) in enumerate(prepared)
    ]


def block_copy(rad_hbm, rad_ref, sems, i):
    lines = pl.ds(pl.multiple_of(i * BLOCK, BLOCK), BLOCK)
    return pltpu.make_async_copy(rad_hbm.at[:, lines, :], rad_ref.at[:, lines, :], sems.at[i])


def await_block(rad_hbm, rad_ref, sems, i, ahead):
    @pl.when(i + ahead < STEPS_D)
    def _():
        block_copy(rad_hbm, rad_ref, sems, i + ahead).start()

    block_copy(rad_hbm, rad_ref, sems, i).wait()


def translate_kernel(
    space_ref, centers_ref, table_hbm, history_hbm, dirs_hbm, rad_hbm,
    first_ref, second_ref, twice_ref, scale_ref, recent_ref,
    rad_ref, table_ref, history_ref, dirs_ref, lines_ref, proj_ref, out_ref, small_sems, sems,
):
    me = space_ref[0]
    start = jnp.where(me == CLUSTERS - 1, me + 1, me + 2)
    small = [
        pltpu.make_async_copy(source, target, small_sems.at[i])
        for i, (source, target) in enumerate(
            ((table_hbm, table_ref), (history_hbm, history_ref), (dirs_hbm, dirs_ref))
        )
    ]
    for copy in small:
        copy.start()
    for i in range(AHEAD):
        block_copy(rad_hbm, rad_ref, sems, i).start()
    for copy in small:
        copy.wait()
    recent_ref[...] = history_ref[0:8, :]
    for axis in range(3):
        for row in range(ROWS):
            lines_ref[axis * ROWS + row : axis * ROWS + row + 1, :] = dirs_ref[
                axis : axis + 1, row * 128 : (row + 1) * 128
            ]
    projected = jnp.dot(
        table_ref[...], history_ref[...], precision=lax.Precision.HIGHEST,
        preferred_element_type=F32,
    )
    for box in range(BOXES_HERE):
        high, low = split_two(projected[:, box * PB : (box + 1) * PB].T)
        proj_ref[box * PB : (box + 1) * PB, 0:128] = high
        proj_ref[box * PB : (box + 1) * PB, 128:256] = low
        proj_ref[(box + 4) * PB : (box + 5) * PB, 0:128] = high
        proj_ref[(box + 4) * PB : (box + 5) * PB, 128:256] = jnp.zeros((PB, 128), BF16)

    def chunk(i, _):
        first_line = pl.multiple_of(i * BLOCK, BLOCK)
        await_block(rad_hbm, rad_ref, sems, i, AHEAD)
        splits = [split_two(rad_ref[box, pl.ds(first_line, BLOCK), :]) for box in range(BOXES_HERE)]
        pieces = jnp.concatenate([high for high, _ in splits] + [low for _, low in splits], axis=1)
        both = jnp.dot(pieces, proj_ref[...], preferred_element_type=F32)
        total = both[:, :128] + both[:, 128:]
        for tile in range(BLOCK // 128):
            turned = total[tile * 128 : (tile + 1) * 128, :].T
            for group in range(TAU // 8):
                out_ref[pl.ds(group * 8 * 9 + tile, 8, stride=9), :] = turned[
                    group * 8 : (group + 1) * 8, :
                ]
                place = pl.ds(group * 8 * LINE + i * 8 + tile, 8, stride=LINE)
                second_ref[place, :] = turned[TAU + group * 8 : TAU + (group + 1) * 8, :]

        rows = pl.ds(pl.multiple_of(i * 8, 8), 8)
        dirs = [
            lines_ref[pl.ds(pl.multiple_of(axis * ROWS + i * 8, 8), 8), :] for axis in range(3)
        ]
        terms_of = lambda m: (out_ref[m * 9 : m * 9 + 8, :],)

        def targets_group(group, _):
            targets = [lax.rem(start + group * 7 + inner, CLUSTERS) for inner in range(7)]
            prepared = [targets_of(me, centers_ref, dirs, target) for target in targets]
            for target, result in zip(targets, clenshaw(terms_of, prepared, 1)):
                first_ref[target, rows, :] = result[0]
            for inner, (twice, scale) in enumerate(prepared):
                twice_ref[group * 7 + inner, rows, :] = twice
                scale_ref[group * 7 + inner, rows, :] = scale
            return 0

        for inner in range(FAR_TARGETS, CLUSTERS):
            first_ref[lax.rem(start + inner, CLUSTERS), rows, :] = jnp.zeros((8, 128), F32)
        lax.fori_loop(0, FAR_TARGETS // 7, targets_group, 0)
        return 0

    lax.fori_loop(0, STEPS_D, chunk, 0)


def in_hbm(x):
    return pltpu.with_memory_space_constraint(x, pltpu.HBM)


def translate(space, centers, history, dirs, radiation):
    smem = pl.BlockSpec(memory_space=pltpu.SMEM)
    hbm = pl.BlockSpec(memory_space=pltpu.HBM)
    vmem = pl.BlockSpec(memory_space=VMEM)
    table = jnp.asarray(projection_table())
    return pl.pallas_call(
        translate_kernel,
        in_specs=[smem, smem, hbm, hbm, hbm, hbm],
        out_specs=[vmem] * 5,
        out_shape=[
            jax.ShapeDtypeStruct((CLUSTERS, ROWS, 128), F32),
            jax.ShapeDtypeStruct((TAU * LINE, 128), F32),
            pltpu.HBM((FAR_TARGETS, ROWS, 128), F32),
            pltpu.HBM((FAR_TARGETS, ROWS, 128), F32),
            jax.ShapeDtypeStruct((8, history.shape[1]), F32),
        ],
        scratch_shapes=[
            VMEM(radiation.shape, F32),
            VMEM((128, K), F32),
            VMEM(history.shape, F32),
            VMEM(dirs.shape, F32),
            VMEM((3 * ROWS, 128), F32),
            VMEM((8 * PB, 256), BF16),
            VMEM((TAU * 9, 128), F32),
            pltpu.SemaphoreType.DMA((3,)),
            pltpu.SemaphoreType.DMA((STEPS_D,)),
        ],
        compiler_params=pltpu.CompilerParams(vmem_limit_bytes=28 << 20),
        cost_estimate=pl.CostEstimate(flops=8 << 30, bytes_accessed=20 << 20, transcendentals=0),
        name="translate",
    )(space, in_hbm(centers), in_hbm(table), in_hbm(history), in_hbm(dirs), in_hbm(radiation))


def known_kernel(space_ref, out_ref, twice_ref, scale_ref, second_ref, weight_ref):
    me = space_ref[0]
    start = jnp.where(me == CLUSTERS - 1, me + 1, me + 2)
    basis_first = basis_table()[:, 0]

    def block(i, _):
        rows = pl.ds(pl.multiple_of(i * 8, 8), 8)
        terms_of = lambda m: (
            out_ref[pl.ds(pl.multiple_of(m * LINE + i * 8, 8), 8), :],
            float(basis_first[m]),
        )

        def targets_group(group, _):
            first = group * 7
            prepared = [
                (twice_ref[first + inner, rows, :], scale_ref[first + inner, rows, :])
                for inner in range(7)
            ]
            for inner, result in enumerate(clenshaw(terms_of, prepared, 2)):
                target = lax.rem(start + first + inner, CLUSTERS)
                second_ref[target, rows, :] = result[0]
                weight_ref[target, rows, :] = result[1]
            return 0

        lax.fori_loop(0, FAR_TARGETS // 7, targets_group, 0)
        for inner in range(FAR_TARGETS, CLUSTERS):
            target = lax.rem(start + inner, CLUSTERS)
            second_ref[target, rows, :] = jnp.zeros((8, 128), F32)
            weight_ref[target, rows, :] = jnp.zeros((8, 128), F32)
        return 0

    lax.fori_loop(0, STEPS_D, block, 0)


def known_part(space, out, twice, scale):
    smem = pl.BlockSpec(memory_space=pltpu.SMEM)
    vmem = pl.BlockSpec(memory_space=VMEM)
    shape = jax.ShapeDtypeStruct((CLUSTERS, ROWS, 128), F32)
    return pl.pallas_call(
        known_kernel,
        in_specs=[smem, vmem, vmem, vmem],
        out_specs=[vmem, vmem],
        out_shape=[shape, shape],
        compiler_params=pltpu.CompilerParams(vmem_limit_bytes=8 << 20),
        cost_estimate=pl.CostEstimate(flops=20 << 20, bytes_accessed=4 << 20, transcendentals=0),
        name="known_part",
    )(space, out, twice, scale)


def near_kernel(
    first_box_ref, nb_ref, counts_ref, excite_ref, lower_ref, own_ref, upper_ref, mats_ref, out_ref, win_ref
):
    box = pl.program_id(0)

    @pl.when(box == 0)
    def _():
        for k in range(KN):
            for place, ref in enumerate((lower_ref, own_ref, upper_ref)):
                for inner in range(BOXES_HERE):
                    row = (place * BOXES_HERE + inner) * 8 + k
                    win_ref[row : row + 1, :] = ref[k : k + 1, inner * PB : (inner + 1) * PB]

    first = jnp.zeros((128, 128), F32)
    second = jnp.zeros((128, 128), F32)
    for j in range(NB):
        place = (nb_ref[box, j] - first_box_ref[0] + BOXES_HERE) * 8
        rows = [win_ref[pl.ds(place + k, 1), :] for k in range(KN)]
        for k in range(KN):
            first = first + mats_ref[0, j, k] * rows[k]
            if k:
                second = second + mats_ref[0, j, k] * rows[k - 1]
    out_ref[pl.ds(box, 1), :] = excite_ref[0:1, :] - row_of_sums(first)
    out_ref[pl.ds(box + BOXES_HERE, 1), :] = excite_ref[1:2, :] - row_of_sums(second)
    live = lax.broadcasted_iota(jnp.int32, (1, PB), 1) < counts_ref[box]
    out_ref[pl.ds(box + 2 * BOXES_HERE, 1), :] = jnp.where(live, 1.0, 0.0)


def near_fields(first_box, neighbours, counts, excite, lower, recent, upper, near_mats):
    smem = pl.BlockSpec(memory_space=pltpu.SMEM)
    side = pl.BlockSpec((8, BOXES_HERE * PB), lambda i: (0, 0))
    return pl.pallas_call(
        near_kernel,
        grid=(BOXES_HERE,),
        in_specs=[
            smem,
            smem,
            smem,
            pl.BlockSpec((STEPS, PB), lambda i: (0, i)),
            side,
            side,
            side,
            pl.BlockSpec((1, NB, KN, PB, PB), lambda i: (i, 0, 0, 0, 0)),
        ],
        out_specs=pl.BlockSpec((16, PB), lambda i: (0, 0)),
        out_shape=jax.ShapeDtypeStruct((16, PB), F32),
        scratch_shapes=[VMEM((3 * BOXES_HERE * 8, PB), F32)],
        compiler_params=pltpu.CompilerParams(vmem_limit_bytes=6 << 20),
        cost_estimate=pl.CostEstimate(flops=1 << 30, bytes_accessed=7 << 20, transcendentals=0),
        name="near_fields",
    )(first_box, neighbours, counts, excite, lower, recent, upper, in_hbm(near_mats))


def near_again_kernel(
    first_box_ref, nb_ref, lower_ref, own_ref, upper_ref, before_ref, mats_ref, out_ref, win_ref
):
    box = pl.program_id(0)

    @pl.when(box == 0)
    def _():
        for place, ref in enumerate((lower_ref, own_ref, upper_ref)):
            win_ref[place * BOXES_HERE : (place + 1) * BOXES_HERE, :] = ref[...]

    total = jnp.zeros((128, 128), F32)
    for j in range(NB):
        place = nb_ref[box, j] - first_box_ref[0] + BOXES_HERE
        total = total + mats_ref[0, j, 0] * win_ref[pl.ds(place, 1), :]
    out_ref[pl.ds(box, 1), :] = before_ref[pl.ds(box + BOXES_HERE, 1), :] - row_of_sums(total)
    out_ref[pl.ds(box + 2 * BOXES_HERE, 1), :] = before_ref[pl.ds(box + 2 * BOXES_HERE, 1), :]


def near_again(first_box, neighbours, lower, own, upper, before, near_mats):
    smem = pl.BlockSpec(memory_space=pltpu.SMEM)
    side = pl.BlockSpec((BOXES_HERE, PB), lambda i: (0, 0))
    return pl.pallas_call(
        near_again_kernel,
        grid=(BOXES_HERE,),
        in_specs=[
            smem,
            smem,
            side,
            side,
            side,
            pl.BlockSpec((16, PB), lambda i: (0, 0)),
            pl.BlockSpec((1, NB, 1, PB, PB), lambda i: (i, 0, 0, 0, 0)),
        ],
        out_specs=pl.BlockSpec((16, PB), lambda i: (0, 0)),
        out_shape=jax.ShapeDtypeStruct((16, PB), F32),
        scratch_shapes=[VMEM((16, PB), F32)],
        compiler_params=pltpu.CompilerParams(vmem_limit_bytes=6 << 20),
        cost_estimate=pl.CostEstimate(flops=1 << 29, bytes_accessed=3 << 20, transcendentals=0),
        name="near_again",
    )(first_box, neighbours, lower, own, upper, before, in_hbm(near_mats))


def far_of_block(samp_ref, rows, rad, sums, ones):
    eye = identity_mask()
    for tile in range(BLOCK // 128):
        row = samp_ref[pl.ds(rows + tile, 1), :]
        high = row.astype(BF16).astype(F32)
        low = row - high
        spread = jnp.concatenate(
            [jnp.where(eye, high, 0.0).astype(BF16), jnp.where(eye, low, 0.0).astype(BF16)], axis=1
        )
        copies = jnp.dot(spread, ones, preferred_element_type=F32)
        for box in range(BOXES_HERE):
            product = rad(box, tile) * copies
            sums[box] = sums[box] + jnp.sum(product.reshape(16, 8, 128), axis=0)
    return sums


def solve(near_ref, inverse_ref, right_side, box):
    solved = row_of_sums(inverse_ref[box] * right_side)
    live = near_ref[2 * BOXES_HERE + box : 2 * BOXES_HERE + box + 1, :] > 0.5
    return jnp.where(live, solved, 0.0)


def far_of_all(samp_ref, parts_ref, rad_hbm, rad_ref, sems):
    for i in range(AHEAD_FAR):
        block_copy(rad_hbm, rad_ref, sems, i).start()
    samp_ref[...] = jnp.sum(parts_ref[...], axis=0)
    ones = jnp.ones((256, 128), BF16)

    def block(i, sums):
        first_line = pl.multiple_of(i * BLOCK, BLOCK)
        await_block(rad_hbm, rad_ref, sems, i, AHEAD_FAR)
        rad = lambda box, tile: rad_ref[
            box, pl.ds(pl.multiple_of(first_line + tile * 128, 128), 128), :
        ]
        return tuple(far_of_block(samp_ref, i * 8, rad, list(sums), ones))

    zero = jnp.zeros((8, 128), F32)
    return lax.fori_loop(0, STEPS_D, block, (zero,) * BOXES_HERE)


def first_step_kernel(
    parts_ref, near_ref, inverse_ref, second_ref, weight_ref, rad_hbm,
    current_ref, field_ref, rad_ref, samp_ref, dot_ref, sems,
):
    sums = far_of_all(samp_ref, parts_ref, rad_hbm, rad_ref, sems)
    ones = jnp.ones((256, 128), BF16)
    currents = []
    for box in range(BOXES_HERE):
        far = jnp.sum(sums[box], axis=0, keepdims=True)
        right_side = near_ref[box : box + 1, :] - far
        current = solve(near_ref, inverse_ref, right_side, box)
        current_ref[box : box + 1, :] = current
        currents.append(current)
    eye = identity_mask()

    def one_block(i, _):
        for tile in range(BLOCK // 128):
            start = pl.multiple_of(i * BLOCK + tile * 128, 128)
            product = rad_ref[0, pl.ds(start, 128), :] * currents[0]
            for box in range(1, BOXES_HERE):
                product = product + rad_ref[box, pl.ds(start, 128), :] * currents[box]
            high, low = split_two(product)
            copies_of = jnp.dot(
                jnp.concatenate([high, low], axis=1), ones, preferred_element_type=F32
            )
            dot_ref[tile : tile + 1, :] = jnp.sum(
                jnp.where(eye, copies_of, 0.0), axis=0, keepdims=True
            )
        response = dot_ref[...]
        rows = pl.ds(pl.multiple_of(i * 8, 8), 8)
        for target in range(CLUSTERS):
            field_ref[target, rows, :] = (
                second_ref[target, rows, :] + weight_ref[target, rows, :] * response
            )
        return 0

    lax.fori_loop(0, STEPS_D, one_block, 0)


def first_step(parts, near, self_inverse, second, weight, radiation):
    vmem = pl.BlockSpec(memory_space=VMEM)
    return pl.pallas_call(
        first_step_kernel,
        in_specs=[vmem] * 5 + [pl.BlockSpec(memory_space=pltpu.HBM)],
        out_specs=[vmem, vmem],
        out_shape=[
            jax.ShapeDtypeStruct((BOXES_HERE, PB), F32),
            jax.ShapeDtypeStruct((CLUSTERS, ROWS, 128), F32),
        ],
        scratch_shapes=[
            VMEM(radiation.shape, F32),
            VMEM((ROWS, 128), F32),
            VMEM((8, 128), F32),
            pltpu.SemaphoreType.DMA((STEPS_D,)),
        ],
        compiler_params=pltpu.CompilerParams(vmem_limit_bytes=28 << 20),
        cost_estimate=pl.CostEstimate(flops=4 << 30, bytes_accessed=20 << 20, transcendentals=0),
        name="first_step",
    )(parts, near, self_inverse, second, weight, in_hbm(radiation))


def second_step_kernel(
    parts_ref, near_ref, inverse_ref, before_ref, rad_hbm,
    out_ref, rad_ref, samp_ref, sems,
):
    sums = far_of_all(samp_ref, parts_ref, rad_hbm, rad_ref, sems)
    for box in range(BOXES_HERE):
        lanes = slice(box * PB, (box + 1) * PB)
        far = jnp.sum(sums[box], axis=0, keepdims=True)
        right_side = near_ref[box : box + 1, :] - far
        out_ref[0:1, lanes] = before_ref[box : box + 1, :]
        out_ref[1:2, lanes] = solve(near_ref, inverse_ref, right_side, box)


def second_step(parts, near, self_inverse, before, radiation):
    vmem = pl.BlockSpec(memory_space=VMEM)
    return pl.pallas_call(
        second_step_kernel,
        in_specs=[vmem] * 4 + [pl.BlockSpec(memory_space=pltpu.HBM)],
        out_specs=vmem,
        out_shape=jax.ShapeDtypeStruct((STEPS, BOXES_HERE * PB), F32),
        scratch_shapes=[
            VMEM(radiation.shape, F32),
            VMEM((ROWS, 128), F32),
            pltpu.SemaphoreType.DMA((STEPS_D,)),
        ],
        compiler_params=pltpu.CompilerParams(vmem_limit_bytes=28 << 20),
        cost_estimate=pl.CostEstimate(flops=4 << 30, bytes_accessed=20 << 20, transcendentals=0),
        name="second_step",
    )(parts, near, self_inverse, before, in_hbm(radiation))


def from_behind(array, by):
    axis = ("space", "ray")
    size = lax.axis_size(axis)
    pairs = [(i, i + by) for i in range(size) if 0 <= i + by < size]
    return lax.ppermute(array, axis, pairs)


def sum_kernel(arrived_ref, copies_ref):
    total = jnp.sum(arrived_ref[...], axis=0)
    for copy in range(copies_ref.shape[0]):
        copies_ref[copy] = total


def summed_copies(arrived, copies):
    vmem = pl.BlockSpec(memory_space=VMEM)
    return pl.pallas_call(
        sum_kernel,
        in_specs=[vmem],
        out_specs=vmem,
        out_shape=jax.ShapeDtypeStruct((copies, *arrived.shape[1:]), F32),
        compiler_params=pltpu.CompilerParams(vmem_limit_bytes=4 << 20),
        cost_estimate=pl.CostEstimate(flops=1 << 17, bytes_accessed=1 << 20, transcendentals=0),
        name="summed_copies",
    )(arrived)


def gathered(field, beside):
    arrived = lax.all_to_all(field, "space", split_axis=0, concat_axis=0, tiled=True)
    copies = summed_copies(arrived, lax.axis_size("ray"))
    copies, beside = lax.optimization_barrier((copies, beside))
    return lax.all_to_all(copies, "ray", split_axis=0, concat_axis=0, tiled=True), beside


def local(
    excite, history, near_mats, neighbours, self_inverse, radiation, directions, centers, counts
):
    space = lax.axis_index("space").astype(jnp.int32).reshape(1)
    first_box = (lax.axis_index(("space", "ray")) * BOXES_HERE).astype(jnp.int32).reshape(1)
    first, out, twice, scale, recent = translate(space, centers, history, directions, radiation)
    lower, upper = from_behind(recent, 1), from_behind(recent, -1)
    second, weight = known_part(space, out, twice, scale)
    parts, (lower, upper, second, weight) = gathered(first, (lower, upper, second, weight))
    near = near_fields(
        first_box, neighbours, counts, excite, lower, recent, upper, near_mats
    )
    current, field = first_step(parts, near, self_inverse, second, weight, radiation)
    lower, upper = from_behind(current, 1), from_behind(current, -1)
    parts, (lower, upper) = gathered(field, (lower, upper))
    near = near_again(first_box, neighbours, lower, current, upper, near, near_mats)
    return second_step(parts, near, self_inverse, current, radiation)


def solution(mesh):
    placed = (
        P(None, ("space", "ray")),
        P(None, ("space", "ray")),
        P(("space", "ray"), None, None, None, None),
        P(("space", "ray"), None),
        P(("space", "ray"), None, None),
        P(("space", "ray"), None, None),
        P(),
        P(),
        P(("space", "ray")),
    )
    return jax.shard_map(
        local, mesh=mesh, in_specs=placed, out_specs=P(None, ("space", "ray")), check_vma=False
    )
```

```python
import math

import jax
import jax.numpy as jnp
import numpy as np
from jax import lax
from jax.experimental import pallas as pl
from jax.experimental.pallas import tpu as pltpu
from jax.sharding import PartitionSpec as P


PB = 128
K = 64
TAU = 48
KN = 3
STEPS = 2
NB = 8
BOXES_HERE = 4
CLUSTERS = 16
FAR_TARGETS = 14
RAYS = 8192
ROWS = RAYS // 128
LINE = ROWS + 8
BLOCK = 1024
STEPS_D = RAYS // BLOCK
AHEAD = 2
AHEAD_FAR = 8
REACH = 2.0 * CLUSTERS + 4.0
VMEM = pltpu.VMEM
F32 = jnp.float32
BF16 = jnp.bfloat16


def basis_table():
    m = np.arange(TAU)[:, None] + 0.5
    k = np.arange(K)[None, :] + 0.5
    return np.sqrt(2.0 / K) * np.cos(np.pi * m * k / K)


def projection_table():
    basis = basis_table()
    table = np.zeros((128, K))
    table[:TAU] = basis
    table[TAU : 2 * TAU, : K - 1] = basis[:, 1:]
    return table.astype(np.float32)


def split_two(x):
    high = x.astype(BF16)
    return high, (x - high.astype(F32)).astype(BF16)


def identity_mask():
    return lax.broadcasted_iota(jnp.int32, (128, 128), 0) == lax.broadcasted_iota(
        jnp.int32, (128, 128), 1
    )


def row_of_sums(matrix):
    return jnp.sum(matrix.T, axis=0, keepdims=True)


def targets_of(me, centers_ref, dirs, target):
    dx, dy, dz = dirs
    sx = centers_ref[0, target] - centers_ref[0, me]
    sy = centers_ref[1, target] - centers_ref[1, me]
    sz = centers_ref[2, target] - centers_ref[2, me]
    squared = jnp.full((8, 128), sx * sx + sy * sy + sz * sz, F32)
    distant = jnp.abs(target - me) >= 2
    inverse = 1.0 / jnp.sqrt(jnp.where(distant, squared, 1.0))
    along = dx * sx + dy * sy + dz * sz
    u = (math.pi / 128.0) * (0.5 + along * (24.0 / REACH))
    v = u * u
    sin = u * (1 + v * (-1 / 6 + v * (1 / 120 + v * (-1 / 5040 + v * (1 / 362880)))))
    cos = 1 + v * (-1 / 2 + v * (1 / 24 + v * (-1 / 720 + v * (1 / 40320))))
    gain = (1.0 + along * inverse) * inverse * (0.5 * math.sqrt(2.0 / K) / math.sqrt(2.0))
    return -4.0 * sin * cos, jnp.where(distant, gain * (cos - sin), 0.0)


def clenshaw(terms_of, prepared, parts):
    zero = jnp.zeros((8, 128), F32)
    ones = [[zero] * parts for _ in prepared]
    twos = [[zero] * parts for _ in prepared]
    for m in reversed(range(TAU)):
        terms = terms_of(m)
        for inner, (twice, _) in enumerate(prepared):
            for part in range(parts):
                new = (terms[part] - twos[inner][part]) + twice * ones[inner][part]
                twos[inner][part] = ones[inner][part]
                ones[inner][part] = new
    return [
        [scale * (one - two) for one, two in zip(ones[inner], twos[inner])]
        for inner, (_, scale) in enumerate(prepared)
    ]


def block_copy(rad_hbm, rad_ref, sems, i):
    lines = pl.ds(pl.multiple_of(i * BLOCK, BLOCK), BLOCK)
    return pltpu.make_async_copy(rad_hbm.at[:, lines, :], rad_ref.at[:, lines, :], sems.at[i])


def await_block(rad_hbm, rad_ref, sems, i, ahead):
    @pl.when(i + ahead < STEPS_D)
    def _():
        block_copy(rad_hbm, rad_ref, sems, i + ahead).start()

    block_copy(rad_hbm, rad_ref, sems, i).wait()


def translate_kernel(
    space_ref, centers_ref, table_hbm, history_hbm, dirs_hbm, rad_hbm,
    first_ref, second_ref, twice_ref, scale_ref,
    rad_ref, table_ref, history_ref, dirs_ref, lines_ref, proj_ref, out_ref, small_sems, sems,
):
    me = space_ref[0]
    start = jnp.where(me == CLUSTERS - 1, me + 1, me + 2)
    small = [
        pltpu.make_async_copy(source, target, small_sems.at[i])
        for i, (source, target) in enumerate(
            ((table_hbm, table_ref), (history_hbm, history_ref), (dirs_hbm, dirs_ref))
        )
    ]
    for copy in small:
        copy.start()
    for i in range(AHEAD):
        block_copy(rad_hbm, rad_ref, sems, i).start()
    for copy in small:
        copy.wait()
    for axis in range(3):
        for row in range(ROWS):
            lines_ref[axis * ROWS + row : axis * ROWS + row + 1, :] = dirs_ref[
                axis : axis + 1, row * 128 : (row + 1) * 128
            ]
    projected = jnp.dot(
        table_ref[...], history_ref[...], precision=lax.Precision.HIGHEST,
        preferred_element_type=F32,
    )
    for box in range(BOXES_HERE):
        high, low = split_two(projected[:, box * PB : (box + 1) * PB].T)
        proj_ref[box * PB : (box + 1) * PB, 0:128] = high
        proj_ref[box * PB : (box + 1) * PB, 128:256] = low
        proj_ref[(box + 4) * PB : (box + 5) * PB, 0:128] = high
        proj_ref[(box + 4) * PB : (box + 5) * PB, 128:256] = jnp.zeros((PB, 128), BF16)

    def chunk(i, _):
        first_line = pl.multiple_of(i * BLOCK, BLOCK)
        await_block(rad_hbm, rad_ref, sems, i, AHEAD)
        splits = [split_two(rad_ref[box, pl.ds(first_line, BLOCK), :]) for box in range(BOXES_HERE)]
        pieces = jnp.concatenate([high for high, _ in splits] + [low for _, low in splits], axis=1)
        both = jnp.dot(pieces, proj_ref[...], preferred_element_type=F32)
        total = both[:, :128] + both[:, 128:]
        for tile in range(BLOCK // 128):
            turned = total[tile * 128 : (tile + 1) * 128, :].T
            for group in range(TAU // 8):
                out_ref[pl.ds(group * 8 * 9 + tile, 8, stride=9), :] = turned[
                    group * 8 : (group + 1) * 8, :
                ]
                place = pl.ds(group * 8 * LINE + i * 8 + tile, 8, stride=LINE)
                second_ref[place, :] = turned[TAU + group * 8 : TAU + (group + 1) * 8, :]

        rows = pl.ds(pl.multiple_of(i * 8, 8), 8)
        dirs = [
            lines_ref[pl.ds(pl.multiple_of(axis * ROWS + i * 8, 8), 8), :] for axis in range(3)
        ]
        terms_of = lambda m: (out_ref[m * 9 : m * 9 + 8, :],)

        def targets_group(group, _):
            targets = [lax.rem(start + group * 7 + inner, CLUSTERS) for inner in range(7)]
            prepared = [targets_of(me, centers_ref, dirs, target) for target in targets]
            for target, result in zip(targets, clenshaw(terms_of, prepared, 1)):
                first_ref[target, rows, :] = result[0]
            for inner, (twice, scale) in enumerate(prepared):
                twice_ref[group * 7 + inner, rows, :] = twice
                scale_ref[group * 7 + inner, rows, :] = scale
            return 0

        for inner in range(FAR_TARGETS, CLUSTERS):
            first_ref[lax.rem(start + inner, CLUSTERS), rows, :] = jnp.zeros((8, 128), F32)
        lax.fori_loop(0, FAR_TARGETS // 7, targets_group, 0)
        return 0

    lax.fori_loop(0, STEPS_D, chunk, 0)


def in_hbm(x):
    return pltpu.with_memory_space_constraint(x, pltpu.HBM)


def translate(space, centers, history, dirs, radiation):
    smem = pl.BlockSpec(memory_space=pltpu.SMEM)
    hbm = pl.BlockSpec(memory_space=pltpu.HBM)
    vmem = pl.BlockSpec(memory_space=VMEM)
    table = jnp.asarray(projection_table())
    return pl.pallas_call(
        translate_kernel,
        in_specs=[smem, smem, hbm, hbm, hbm, hbm],
        out_specs=[vmem] * 4,
        out_shape=[
            jax.ShapeDtypeStruct((CLUSTERS, ROWS, 128), F32),
            jax.ShapeDtypeStruct((TAU * LINE, 128), F32),
            pltpu.HBM((FAR_TARGETS, ROWS, 128), F32),
            pltpu.HBM((FAR_TARGETS, ROWS, 128), F32),
        ],
        scratch_shapes=[
            VMEM(radiation.shape, F32),
            VMEM((128, K), F32),
            VMEM(history.shape, F32),
            VMEM(dirs.shape, F32),
            VMEM((3 * ROWS, 128), F32),
            VMEM((8 * PB, 256), BF16),
            VMEM((TAU * 9, 128), F32),
            pltpu.SemaphoreType.DMA((3,)),
            pltpu.SemaphoreType.DMA((STEPS_D,)),
        ],
        compiler_params=pltpu.CompilerParams(vmem_limit_bytes=28 << 20),
        cost_estimate=pl.CostEstimate(flops=8 << 30, bytes_accessed=20 << 20, transcendentals=0),
        name="translate",
    )(space, in_hbm(centers), in_hbm(table), in_hbm(history), in_hbm(dirs), in_hbm(radiation))


def known_kernel(space_ref, out_ref, twice_ref, scale_ref, second_ref, weight_ref):
    me = space_ref[0]
    start = jnp.where(me == CLUSTERS - 1, me + 1, me + 2)
    basis_first = basis_table()[:, 0]

    def block(i, _):
        rows = pl.ds(pl.multiple_of(i * 8, 8), 8)
        terms_of = lambda m: (
            out_ref[pl.ds(pl.multiple_of(m * LINE + i * 8, 8), 8), :],
            float(basis_first[m]),
        )

        def targets_group(group, _):
            first = group * 7
            prepared = [
                (twice_ref[first + inner, rows, :], scale_ref[first + inner, rows, :])
                for inner in range(7)
            ]
            for inner, result in enumerate(clenshaw(terms_of, prepared, 2)):
                target = lax.rem(start + first + inner, CLUSTERS)
                second_ref[target, rows, :] = result[0]
                weight_ref[target, rows, :] = result[1]
            return 0

        lax.fori_loop(0, FAR_TARGETS // 7, targets_group, 0)
        for inner in range(FAR_TARGETS, CLUSTERS):
            target = lax.rem(start + inner, CLUSTERS)
            second_ref[target, rows, :] = jnp.zeros((8, 128), F32)
            weight_ref[target, rows, :] = jnp.zeros((8, 128), F32)
        return 0

    lax.fori_loop(0, STEPS_D, block, 0)


def known_part(space, out, twice, scale):
    smem = pl.BlockSpec(memory_space=pltpu.SMEM)
    vmem = pl.BlockSpec(memory_space=VMEM)
    shape = pltpu.HBM((CLUSTERS, ROWS, 128), F32)
    return pl.pallas_call(
        known_kernel,
        in_specs=[smem, vmem, vmem, vmem],
        out_specs=[vmem, vmem],
        out_shape=[shape, shape],
        compiler_params=pltpu.CompilerParams(vmem_limit_bytes=8 << 20),
        cost_estimate=pl.CostEstimate(flops=20 << 20, bytes_accessed=4 << 20, transcendentals=0),
        name="known_part",
    )(space, out, in_hbm(twice), in_hbm(scale))


def near_kernel(
    first_box_ref, nb_ref, counts_ref, excite_ref, lower_ref, own_ref, upper_ref, mats_ref, out_ref, win_ref
):
    box = pl.program_id(0)

    @pl.when(box == 0)
    def _():
        for k in range(KN):
            for place, ref in enumerate((lower_ref, own_ref, upper_ref)):
                for inner in range(BOXES_HERE):
                    row = (place * BOXES_HERE + inner) * 8 + k
                    win_ref[row : row + 1, :] = ref[k : k + 1, inner * PB : (inner + 1) * PB]

    first = jnp.zeros((128, 128), F32)
    second = jnp.zeros((128, 128), F32)
    for j in range(NB):
        place = (nb_ref[box, j] - first_box_ref[0] + BOXES_HERE) * 8
        rows = [win_ref[pl.ds(place + k, 1), :] for k in range(KN)]
        for k in range(KN):
            first = first + mats_ref[0, j, k] * rows[k]
            if k:
                second = second + mats_ref[0, j, k] * rows[k - 1]
    out_ref[pl.ds(box, 1), :] = excite_ref[0:1, :] - row_of_sums(first)
    out_ref[pl.ds(box + BOXES_HERE, 1), :] = excite_ref[1:2, :] - row_of_sums(second)
    live = lax.broadcasted_iota(jnp.int32, (1, PB), 1) < counts_ref[box]
    out_ref[pl.ds(box + 2 * BOXES_HERE, 1), :] = jnp.where(live, 1.0, 0.0)


def near_fields(first_box, neighbours, counts, excite, lower, recent, upper, near_mats):
    smem = pl.BlockSpec(memory_space=pltpu.SMEM)
    side = pl.BlockSpec((8, BOXES_HERE * PB), lambda i: (0, 0))
    return pl.pallas_call(
        near_kernel,
        grid=(BOXES_HERE,),
        in_specs=[
            smem,
            smem,
            smem,
            pl.BlockSpec((STEPS, PB), lambda i: (0, i)),
            side,
            side,
            side,
            pl.BlockSpec((1, NB, KN, PB, PB), lambda i: (i, 0, 0, 0, 0)),
        ],
        out_specs=pl.BlockSpec((16, PB), lambda i: (0, 0)),
        out_shape=jax.ShapeDtypeStruct((16, PB), F32),
        scratch_shapes=[VMEM((3 * BOXES_HERE * 8, PB), F32)],
        compiler_params=pltpu.CompilerParams(vmem_limit_bytes=6 << 20),
        cost_estimate=pl.CostEstimate(flops=1 << 30, bytes_accessed=7 << 20, transcendentals=0),
        name="near_fields",
    )(first_box, neighbours, counts, excite, lower, recent, upper, in_hbm(near_mats))


def near_again_kernel(
    first_box_ref, nb_ref, lower_ref, own_ref, upper_ref, before_ref, mats_ref, out_ref, win_ref
):
    box = pl.program_id(0)

    @pl.when(box == 0)
    def _():
        for place, ref in enumerate((lower_ref, own_ref, upper_ref)):
            win_ref[place * BOXES_HERE : (place + 1) * BOXES_HERE, :] = ref[...]

    total = jnp.zeros((128, 128), F32)
    for j in range(NB):
        place = nb_ref[box, j] - first_box_ref[0] + BOXES_HERE
        total = total + mats_ref[0, j, 0] * win_ref[pl.ds(place, 1), :]
    out_ref[pl.ds(box, 1), :] = before_ref[pl.ds(box + BOXES_HERE, 1), :] - row_of_sums(total)
    out_ref[pl.ds(box + 2 * BOXES_HERE, 1), :] = before_ref[pl.ds(box + 2 * BOXES_HERE, 1), :]


def near_again(first_box, neighbours, lower, own, upper, before, near_mats):
    smem = pl.BlockSpec(memory_space=pltpu.SMEM)
    side = pl.BlockSpec((BOXES_HERE, PB), lambda i: (0, 0))
    return pl.pallas_call(
        near_again_kernel,
        grid=(BOXES_HERE,),
        in_specs=[
            smem,
            smem,
            side,
            side,
            side,
            pl.BlockSpec((16, PB), lambda i: (0, 0)),
            pl.BlockSpec((1, NB, 1, PB, PB), lambda i: (i, 0, 0, 0, 0)),
        ],
        out_specs=pl.BlockSpec((16, PB), lambda i: (0, 0)),
        out_shape=jax.ShapeDtypeStruct((16, PB), F32),
        scratch_shapes=[VMEM((16, PB), F32)],
        compiler_params=pltpu.CompilerParams(vmem_limit_bytes=6 << 20),
        cost_estimate=pl.CostEstimate(flops=1 << 29, bytes_accessed=3 << 20, transcendentals=0),
        name="near_again",
    )(first_box, neighbours, lower, own, upper, before, in_hbm(near_mats))


def far_of_block(samp_ref, rows, rad, sums, ones):
    eye = identity_mask()
    for tile in range(BLOCK // 128):
        row = samp_ref[pl.ds(rows + tile, 1), :]
        high = row.astype(BF16).astype(F32)
        low = row - high
        spread = jnp.concatenate(
            [jnp.where(eye, high, 0.0).astype(BF16), jnp.where(eye, low, 0.0).astype(BF16)], axis=1
        )
        copies = jnp.dot(spread, ones, preferred_element_type=F32)
        for box in range(BOXES_HERE):
            product = rad(box, tile) * copies
            sums[box] = sums[box] + jnp.sum(product.reshape(16, 8, 128), axis=0)
    return sums


def solve(near_ref, inverse_ref, right_side, box):
    solved = row_of_sums(inverse_ref[box] * right_side)
    live = near_ref[2 * BOXES_HERE + box : 2 * BOXES_HERE + box + 1, :] > 0.5
    return jnp.where(live, solved, 0.0)


def far_of_all(samp_ref, parts_ref, rad_hbm, rad_ref, sems):
    for i in range(AHEAD_FAR):
        block_copy(rad_hbm, rad_ref, sems, i).start()
    samp_ref[...] = jnp.sum(parts_ref[...], axis=0)
    ones = jnp.ones((256, 128), BF16)

    def block(i, sums):
        first_line = pl.multiple_of(i * BLOCK, BLOCK)
        await_block(rad_hbm, rad_ref, sems, i, AHEAD_FAR)
        rad = lambda box, tile: rad_ref[
            box, pl.ds(pl.multiple_of(first_line + tile * 128, 128), 128), :
        ]
        return tuple(far_of_block(samp_ref, i * 8, rad, list(sums), ones))

    zero = jnp.zeros((8, 128), F32)
    return lax.fori_loop(0, STEPS_D, block, (zero,) * BOXES_HERE)


def first_step_kernel(
    parts_ref, near_ref, inverse_ref, second_ref, weight_ref, rad_hbm,
    current_ref, field_ref, rad_ref, samp_ref, dot_ref, sems,
):
    sums = far_of_all(samp_ref, parts_ref, rad_hbm, rad_ref, sems)
    ones = jnp.ones((256, 128), BF16)
    currents = []
    for box in range(BOXES_HERE):
        far = jnp.sum(sums[box], axis=0, keepdims=True)
        right_side = near_ref[box : box + 1, :] - far
        current = solve(near_ref, inverse_ref, right_side, box)
        current_ref[box : box + 1, :] = current
        currents.append(current)
    eye = identity_mask()

    def one_block(i, _):
        for tile in range(BLOCK // 128):
            start = pl.multiple_of(i * BLOCK + tile * 128, 128)
            product = rad_ref[0, pl.ds(start, 128), :] * currents[0]
            for box in range(1, BOXES_HERE):
                product = product + rad_ref[box, pl.ds(start, 128), :] * currents[box]
            high, low = split_two(product)
            copies_of = jnp.dot(
                jnp.concatenate([high, low], axis=1), ones, preferred_element_type=F32
            )
            dot_ref[tile : tile + 1, :] = jnp.sum(
                jnp.where(eye, copies_of, 0.0), axis=0, keepdims=True
            )
        response = dot_ref[...]
        rows = pl.ds(pl.multiple_of(i * 8, 8), 8)
        for target in range(CLUSTERS):
            field_ref[target, rows, :] = (
                second_ref[target, rows, :] + weight_ref[target, rows, :] * response
            )
        return 0

    lax.fori_loop(0, STEPS_D, one_block, 0)


def first_step(parts, near, self_inverse, second, weight, radiation):
    vmem = pl.BlockSpec(memory_space=VMEM)
    return pl.pallas_call(
        first_step_kernel,
        in_specs=[vmem] * 5 + [pl.BlockSpec(memory_space=pltpu.HBM)],
        out_specs=[vmem, vmem],
        out_shape=[
            jax.ShapeDtypeStruct((BOXES_HERE, PB), F32),
            jax.ShapeDtypeStruct((CLUSTERS, ROWS, 128), F32),
        ],
        scratch_shapes=[
            VMEM(radiation.shape, F32),
            VMEM((ROWS, 128), F32),
            VMEM((8, 128), F32),
            pltpu.SemaphoreType.DMA((STEPS_D,)),
        ],
        compiler_params=pltpu.CompilerParams(vmem_limit_bytes=28 << 20),
        cost_estimate=pl.CostEstimate(flops=4 << 30, bytes_accessed=20 << 20, transcendentals=0),
        name="first_step",
    )(parts, near, self_inverse, second, weight, in_hbm(radiation))


def second_step_kernel(
    parts_ref, near_ref, inverse_ref, before_ref, rad_hbm,
    out_ref, rad_ref, samp_ref, sems,
):
    sums = far_of_all(samp_ref, parts_ref, rad_hbm, rad_ref, sems)
    for box in range(BOXES_HERE):
        lanes = slice(box * PB, (box + 1) * PB)
        far = jnp.sum(sums[box], axis=0, keepdims=True)
        right_side = near_ref[box : box + 1, :] - far
        out_ref[0:1, lanes] = before_ref[box : box + 1, :]
        out_ref[1:2, lanes] = solve(near_ref, inverse_ref, right_side, box)


def second_step(parts, near, self_inverse, before, radiation):
    vmem = pl.BlockSpec(memory_space=VMEM)
    return pl.pallas_call(
        second_step_kernel,
        in_specs=[vmem] * 4 + [pl.BlockSpec(memory_space=pltpu.HBM)],
        out_specs=vmem,
        out_shape=jax.ShapeDtypeStruct((STEPS, BOXES_HERE * PB), F32),
        scratch_shapes=[
            VMEM(radiation.shape, F32),
            VMEM((ROWS, 128), F32),
            pltpu.SemaphoreType.DMA((STEPS_D,)),
        ],
        compiler_params=pltpu.CompilerParams(vmem_limit_bytes=28 << 20),
        cost_estimate=pl.CostEstimate(flops=4 << 30, bytes_accessed=20 << 20, transcendentals=0),
        name="second_step",
    )(parts, near, self_inverse, before, in_hbm(radiation))


def from_behind(array, by):
    axis = ("space", "ray")
    size = lax.axis_size(axis)
    pairs = [(i, i + by) for i in range(size) if 0 <= i + by < size]
    return lax.ppermute(array, axis, pairs)


def sum_kernel(arrived_ref, copies_ref):
    total = jnp.sum(arrived_ref[...], axis=0)
    for copy in range(copies_ref.shape[0]):
        copies_ref[copy] = total


def summed_copies(arrived, copies):
    vmem = pl.BlockSpec(memory_space=VMEM)
    return pl.pallas_call(
        sum_kernel,
        in_specs=[vmem],
        out_specs=vmem,
        out_shape=jax.ShapeDtypeStruct((copies, *arrived.shape[1:]), F32),
        compiler_params=pltpu.CompilerParams(vmem_limit_bytes=4 << 20),
        cost_estimate=pl.CostEstimate(flops=1 << 17, bytes_accessed=1 << 20, transcendentals=0),
        name="summed_copies",
    )(arrived)


def gathered(field, beside):
    arrived = lax.all_to_all(field, "space", split_axis=0, concat_axis=0, tiled=True)
    copies = summed_copies(arrived, lax.axis_size("ray"))
    copies, beside = lax.optimization_barrier((copies, beside))
    return lax.all_to_all(copies, "ray", split_axis=0, concat_axis=0, tiled=True), beside


def steps(
    excite, history, near_mats, neighbours, self_inverse, radiation, directions, centers, counts
):
    space = lax.axis_index("space").astype(jnp.int32).reshape(1)
    first_box = (lax.axis_index(("space", "ray")) * BOXES_HERE).astype(jnp.int32).reshape(1)
    recent = history[:8]
    lower = from_behind(recent, 1)
    upper = from_behind(recent, -1)
    first, out, twice, scale = translate(space, centers, history, directions, radiation)
    second, weight = known_part(space, out, twice, scale)
    parts, (lower, upper, second, weight) = gathered(first, (lower, upper, second, weight))
    near = near_fields(
        first_box, neighbours, counts, excite, lower, history, upper, near_mats
    )
    current, field = first_step(parts, near, self_inverse, second, weight, radiation)
    lower, upper = from_behind(current, 1), from_behind(current, -1)
    parts, (lower, upper) = gathered(field, (lower, upper))
    near = near_again(first_box, neighbours, lower, current, upper, near, near_mats)
    return second_step(parts, near, self_inverse, current, radiation)


def solution(mesh):
    placed = (
        P(None, ("space", "ray")),
        P(None, ("space", "ray")),
        P(("space", "ray"), None, None, None, None),
        P(("space", "ray"), None),
        P(("space", "ray"), None, None),
        P(("space", "ray"), None, None),
        P(),
        P(),
        P(("space", "ray")),
    )
    return jax.shard_map(
        steps, mesh=mesh, in_specs=placed, out_specs=P(None, ("space", "ray")), check_vma=False
    )
```

```python
import math

import jax
import jax.numpy as jnp
import numpy as np
from jax import lax
from jax.experimental import pallas as pl
from jax.experimental.pallas import tpu as pltpu
from jax.sharding import PartitionSpec as P


PB = 128
K = 64
TAU = 48
KN = 3
STEPS = 2
NB = 8
BOXES_HERE = 4
CLUSTERS = 16
FAR_TARGETS = 14
RAYS = 8192
ROWS = RAYS // 128
LINE = ROWS + 8
BLOCK = 1024
STEPS_D = RAYS // BLOCK
AHEAD = 2
AHEAD_FAR = 8
REACH = 2.0 * CLUSTERS + 4.0
VMEM = pltpu.VMEM
F32 = jnp.float32
BF16 = jnp.bfloat16


def basis_table():
    m = np.arange(TAU)[:, None] + 0.5
    k = np.arange(K)[None, :] + 0.5
    return np.sqrt(2.0 / K) * np.cos(np.pi * m * k / K)


def projection_table():
    basis = basis_table()
    table = np.zeros((128, K))
    table[:TAU] = basis
    table[TAU : 2 * TAU, : K - 1] = basis[:, 1:]
    return table.astype(np.float32)


def split_two(x):
    high = x.astype(BF16)
    return high, (x - high.astype(F32)).astype(BF16)


def identity_mask():
    return lax.broadcasted_iota(jnp.int32, (128, 128), 0) == lax.broadcasted_iota(
        jnp.int32, (128, 128), 1
    )


def row_of_sums(matrix):
    return jnp.sum(matrix.T, axis=0, keepdims=True)


def targets_of(me, centers_ref, dirs, target):
    dx, dy, dz = dirs
    sx = centers_ref[0, target] - centers_ref[0, me]
    sy = centers_ref[1, target] - centers_ref[1, me]
    sz = centers_ref[2, target] - centers_ref[2, me]
    squared = jnp.full((8, 128), sx * sx + sy * sy + sz * sz, F32)
    distant = jnp.abs(target - me) >= 2
    inverse = 1.0 / jnp.sqrt(jnp.where(distant, squared, 1.0))
    along = dx * sx + dy * sy + dz * sz
    u = (math.pi / 128.0) * (0.5 + along * (24.0 / REACH))
    v = u * u
    sin = u * (1 + v * (-1 / 6 + v * (1 / 120 + v * (-1 / 5040 + v * (1 / 362880)))))
    cos = 1 + v * (-1 / 2 + v * (1 / 24 + v * (-1 / 720 + v * (1 / 40320))))
    gain = (1.0 + along * inverse) * inverse * (0.5 * math.sqrt(2.0 / K) / math.sqrt(2.0))
    return -4.0 * sin * cos, jnp.where(distant, gain * (cos - sin), 0.0)


def clenshaw(terms_of, prepared, parts):
    zero = jnp.zeros((8, 128), F32)
    ones = [[zero] * parts for _ in prepared]
    twos = [[zero] * parts for _ in prepared]
    for m in reversed(range(TAU)):
        terms = terms_of(m)
        for inner, (twice, _) in enumerate(prepared):
            for part in range(parts):
                new = (terms[part] - twos[inner][part]) + twice * ones[inner][part]
                twos[inner][part] = ones[inner][part]
                ones[inner][part] = new
    return [
        [scale * (one - two) for one, two in zip(ones[inner], twos[inner])]
        for inner, (_, scale) in enumerate(prepared)
    ]


def block_rows(first, size):
    return pl.ds(first if isinstance(first, int) else pl.multiple_of(first, size), size)


def block_copy(rad_hbm, rad_ref, sems, i):
    lines = block_rows(i * BLOCK, BLOCK)
    return pltpu.make_async_copy(rad_hbm.at[:, lines, :], rad_ref.at[:, lines, :], sems.at[i])


def await_block(rad_hbm, rad_ref, sems, i, ahead):
    def start():
        block_copy(rad_hbm, rad_ref, sems, i + ahead).start()

    if isinstance(i, int):
        if i + ahead < STEPS_D:
            start()
    else:
        pl.when(i + ahead < STEPS_D)(start)
    block_copy(rad_hbm, rad_ref, sems, i).wait()


def translate_kernel(
    space_ref, centers_ref, table_hbm, history_hbm, dirs_hbm, rad_hbm,
    first_ref, second_ref, twice_ref, scale_ref, recent_ref,
    rad_ref, table_ref, history_ref, dirs_ref, lines_ref, proj_ref, out_ref, odd_ref, small_sems, sems,
):
    me = space_ref[0]
    start = jnp.where(me == CLUSTERS - 1, me + 1, me + 2)
    small = [
        pltpu.make_async_copy(source, target, small_sems.at[i])
        for i, (source, target) in enumerate(
            ((table_hbm, table_ref), (history_hbm, history_ref), (dirs_hbm, dirs_ref))
        )
    ]
    for copy in small:
        copy.start()
    for i in range(AHEAD):
        block_copy(rad_hbm, rad_ref, sems, i).start()
    for copy in small:
        copy.wait()
    recent_ref[...] = history_ref[0:8, :]
    for axis in range(3):
        for row in range(ROWS):
            lines_ref[axis * ROWS + row : axis * ROWS + row + 1, :] = dirs_ref[
                axis : axis + 1, row * 128 : (row + 1) * 128
            ]
    projected = jnp.dot(
        table_ref[...], history_ref[...], precision=lax.Precision.HIGHEST,
        preferred_element_type=F32,
    )
    for box in range(BOXES_HERE):
        high, low = split_two(projected[:, box * PB : (box + 1) * PB].T)
        proj_ref[box * PB : (box + 1) * PB, 0:128] = high
        proj_ref[box * PB : (box + 1) * PB, 128:256] = low
        proj_ref[(box + 4) * PB : (box + 5) * PB, 0:128] = high
        proj_ref[(box + 4) * PB : (box + 5) * PB, 128:256] = jnp.zeros((PB, 128), BF16)

    def project(i, quarter, slot):
        lines = block_rows(i * BLOCK + quarter * 256, 256)
        splits = [split_two(rad_ref[box, lines, :]) for box in range(BOXES_HERE)]
        pieces = jnp.concatenate([high for high, _ in splits] + [low for _, low in splits], axis=1)
        both = jnp.dot(pieces, proj_ref[...], preferred_element_type=F32)
        total = both[:, :128] + both[:, 128:]
        for inner in range(2):
            turned = total[inner * 128 : (inner + 1) * 128, :].T
            tile = quarter * 2 + inner
            for group in range(TAU // 8):
                slot[pl.ds(group * 8 * 9 + tile, 8, stride=9), :] = turned[
                    group * 8 : (group + 1) * 8, :
                ]
                place = pl.ds(group * 8 * LINE + i * 8 + tile, 8, stride=LINE)
                second_ref[place, :] = turned[TAU + group * 8 : TAU + (group + 1) * 8, :]

    def spread(i, quarter, slot):
        rows = block_rows(i * 8, 8)
        dirs = [lines_ref[block_rows(axis * ROWS + i * 8, 8), :] for axis in range(3)]
        places = range(quarter * 4, min(quarter * 4 + 4, FAR_TARGETS))
        targets = [lax.rem(start + place, CLUSTERS) for place in places]
        prepared = [targets_of(me, centers_ref, dirs, target) for target in targets]
        terms_of = lambda m: (slot[m * 9 : m * 9 + 8, :],)
        for target, result in zip(targets, clenshaw(terms_of, prepared, 1)):
            first_ref[target, rows, :] = result[0]
        for place, (twice, scale) in zip(places, prepared):
            twice_ref[place, rows, :] = twice
            scale_ref[place, rows, :] = scale
        if quarter == 3:
            for inner in range(FAR_TARGETS, CLUSTERS):
                first_ref[lax.rem(start + inner, CLUSTERS), rows, :] = jnp.zeros((8, 128), F32)

    def both_of(i, slot, before):
        await_block(rad_hbm, rad_ref, sems, i, AHEAD)
        for quarter in range(4):
            project(i, quarter, slot)
            spread(i - 1, quarter, before)

    def two_blocks(pair, _):
        both_of(2 * pair + 1, odd_ref, out_ref)
        both_of(2 * pair + 2, out_ref, odd_ref)
        return 0

    await_block(rad_hbm, rad_ref, sems, 0, AHEAD)
    for quarter in range(4):
        project(0, quarter, out_ref)
    lax.fori_loop(0, STEPS_D // 2 - 1, two_blocks, 0)
    both_of(STEPS_D - 1, odd_ref, out_ref)
    for quarter in range(4):
        spread(STEPS_D - 1, quarter, odd_ref)


def in_hbm(x):
    return pltpu.with_memory_space_constraint(x, pltpu.HBM)


def translate(space, centers, history, dirs, radiation):
    smem = pl.BlockSpec(memory_space=pltpu.SMEM)
    hbm = pl.BlockSpec(memory_space=pltpu.HBM)
    vmem = pl.BlockSpec(memory_space=VMEM)
    table = jnp.asarray(projection_table())
    return pl.pallas_call(
        translate_kernel,
        in_specs=[smem, smem, hbm, hbm, hbm, hbm],
        out_specs=[vmem] * 5,
        out_shape=[
            jax.ShapeDtypeStruct((CLUSTERS, ROWS, 128), F32),
            jax.ShapeDtypeStruct((TAU * LINE, 128), F32),
            pltpu.HBM((FAR_TARGETS, ROWS, 128), F32),
            pltpu.HBM((FAR_TARGETS, ROWS, 128), F32),
            jax.ShapeDtypeStruct((8, history.shape[1]), F32),
        ],
        scratch_shapes=[
            VMEM(radiation.shape, F32),
            VMEM((128, K), F32),
            VMEM(history.shape, F32),
            VMEM(dirs.shape, F32),
            VMEM((3 * ROWS, 128), F32),
            VMEM((8 * PB, 256), BF16),
            VMEM((TAU * 9, 128), F32),
            VMEM((TAU * 9, 128), F32),
            pltpu.SemaphoreType.DMA((3,)),
            pltpu.SemaphoreType.DMA((STEPS_D,)),
        ],
        compiler_params=pltpu.CompilerParams(vmem_limit_bytes=28 << 20),
        cost_estimate=pl.CostEstimate(flops=8 << 30, bytes_accessed=20 << 20, transcendentals=0),
        name="translate",
    )(space, in_hbm(centers), in_hbm(table), in_hbm(history), in_hbm(dirs), in_hbm(radiation))


def known_kernel(space_ref, out_ref, twice_ref, scale_ref, second_ref, weight_ref):
    me = space_ref[0]
    start = jnp.where(me == CLUSTERS - 1, me + 1, me + 2)
    basis_first = basis_table()[:, 0]

    def block(i, _):
        rows = pl.ds(pl.multiple_of(i * 8, 8), 8)
        terms_of = lambda m: (
            out_ref[pl.ds(pl.multiple_of(m * LINE + i * 8, 8), 8), :],
            float(basis_first[m]),
        )

        def targets_group(group, _):
            first = group * 7
            prepared = [
                (twice_ref[first + inner, rows, :], scale_ref[first + inner, rows, :])
                for inner in range(7)
            ]
            for inner, result in enumerate(clenshaw(terms_of, prepared, 2)):
                target = lax.rem(start + first + inner, CLUSTERS)
                second_ref[target, rows, :] = result[0]
                weight_ref[target, rows, :] = result[1]
            return 0

        lax.fori_loop(0, FAR_TARGETS // 7, targets_group, 0)
        for inner in range(FAR_TARGETS, CLUSTERS):
            target = lax.rem(start + inner, CLUSTERS)
            second_ref[target, rows, :] = jnp.zeros((8, 128), F32)
            weight_ref[target, rows, :] = jnp.zeros((8, 128), F32)
        return 0

    lax.fori_loop(0, STEPS_D, block, 0)


def known_part(space, out, twice, scale):
    smem = pl.BlockSpec(memory_space=pltpu.SMEM)
    vmem = pl.BlockSpec(memory_space=VMEM)
    shape = pltpu.HBM((CLUSTERS, ROWS, 128), F32)
    return pl.pallas_call(
        known_kernel,
        in_specs=[smem, vmem, vmem, vmem],
        out_specs=[vmem, vmem],
        out_shape=[shape, shape],
        compiler_params=pltpu.CompilerParams(vmem_limit_bytes=8 << 20),
        cost_estimate=pl.CostEstimate(flops=20 << 20, bytes_accessed=4 << 20, transcendentals=0),
        name="known_part",
    )(space, out, in_hbm(twice), in_hbm(scale))


def near_kernel(
    first_box_ref, nb_ref, counts_ref, excite_ref, lower_ref, own_ref, upper_ref, mats_ref, out_ref, win_ref
):
    box = pl.program_id(0)

    @pl.when(box == 0)
    def _():
        for k in range(KN):
            for place, ref in enumerate((lower_ref, own_ref, upper_ref)):
                for inner in range(BOXES_HERE):
                    row = (place * BOXES_HERE + inner) * 8 + k
                    win_ref[row : row + 1, :] = ref[k : k + 1, inner * PB : (inner + 1) * PB]

    first = jnp.zeros((128, 128), F32)
    second = jnp.zeros((128, 128), F32)
    for j in range(NB):
        place = (nb_ref[box, j] - first_box_ref[0] + BOXES_HERE) * 8
        rows = [win_ref[pl.ds(place + k, 1), :] for k in range(KN)]
        for k in range(KN):
            first = first + mats_ref[0, j, k] * rows[k]
            if k:
                second = second + mats_ref[0, j, k] * rows[k - 1]
    out_ref[pl.ds(box, 1), :] = excite_ref[0:1, :] - row_of_sums(first)
    out_ref[pl.ds(box + BOXES_HERE, 1), :] = excite_ref[1:2, :] - row_of_sums(second)
    live = lax.broadcasted_iota(jnp.int32, (1, PB), 1) < counts_ref[box]
    out_ref[pl.ds(box + 2 * BOXES_HERE, 1), :] = jnp.where(live, 1.0, 0.0)


def near_fields(first_box, neighbours, counts, excite, lower, recent, upper, near_mats):
    smem = pl.BlockSpec(memory_space=pltpu.SMEM)
    side = pl.BlockSpec((8, BOXES_HERE * PB), lambda i: (0, 0))
    return pl.pallas_call(
        near_kernel,
        grid=(BOXES_HERE,),
        in_specs=[
            smem,
            smem,
            smem,
            pl.BlockSpec((STEPS, PB), lambda i: (0, i)),
            side,
            side,
            side,
            pl.BlockSpec((1, NB, KN, PB, PB), lambda i: (i, 0, 0, 0, 0)),
        ],
        out_specs=pl.BlockSpec((16, PB), lambda i: (0, 0)),
        out_shape=jax.ShapeDtypeStruct((16, PB), F32),
        scratch_shapes=[VMEM((3 * BOXES_HERE * 8, PB), F32)],
        compiler_params=pltpu.CompilerParams(vmem_limit_bytes=6 << 20),
        cost_estimate=pl.CostEstimate(flops=1 << 30, bytes_accessed=7 << 20, transcendentals=0),
        name="near_fields",
    )(first_box, neighbours, counts, excite, lower, recent, upper, in_hbm(near_mats))


def near_again_kernel(
    first_box_ref, nb_ref, lower_ref, own_ref, upper_ref, before_ref, mats_ref, out_ref, win_ref
):
    box = pl.program_id(0)

    @pl.when(box == 0)
    def _():
        for place, ref in enumerate((lower_ref, own_ref, upper_ref)):
            win_ref[place * BOXES_HERE : (place + 1) * BOXES_HERE, :] = ref[...]

    total = jnp.zeros((128, 128), F32)
    for j in range(NB):
        place = nb_ref[box, j] - first_box_ref[0] + BOXES_HERE
        total = total + mats_ref[0, j, 0] * win_ref[pl.ds(place, 1), :]
    out_ref[pl.ds(box, 1), :] = before_ref[pl.ds(box + BOXES_HERE, 1), :] - row_of_sums(total)
    out_ref[pl.ds(box + 2 * BOXES_HERE, 1), :] = before_ref[pl.ds(box + 2 * BOXES_HERE, 1), :]


def near_again(first_box, neighbours, lower, own, upper, before, near_mats):
    smem = pl.BlockSpec(memory_space=pltpu.SMEM)
    side = pl.BlockSpec((BOXES_HERE, PB), lambda i: (0, 0))
    return pl.pallas_call(
        near_again_kernel,
        grid=(BOXES_HERE,),
        in_specs=[
            smem,
            smem,
            side,
            side,
            side,
            pl.BlockSpec((16, PB), lambda i: (0, 0)),
            pl.BlockSpec((1, NB, 1, PB, PB), lambda i: (i, 0, 0, 0, 0)),
        ],
        out_specs=pl.BlockSpec((16, PB), lambda i: (0, 0)),
        out_shape=jax.ShapeDtypeStruct((16, PB), F32),
        scratch_shapes=[VMEM((16, PB), F32)],
        compiler_params=pltpu.CompilerParams(vmem_limit_bytes=6 << 20),
        cost_estimate=pl.CostEstimate(flops=1 << 29, bytes_accessed=3 << 20, transcendentals=0),
        name="near_again",
    )(first_box, neighbours, lower, own, upper, before, in_hbm(near_mats))


def far_of_block(samp_ref, rows, rad, sums, ones):
    eye = identity_mask()
    for tile in range(BLOCK // 128):
        row = samp_ref[pl.ds(rows + tile, 1), :]
        high = row.astype(BF16).astype(F32)
        low = row - high
        spread = jnp.concatenate(
            [jnp.where(eye, high, 0.0).astype(BF16), jnp.where(eye, low, 0.0).astype(BF16)], axis=1
        )
        copies = jnp.dot(spread, ones, preferred_element_type=F32)
        for box in range(BOXES_HERE):
            product = rad(box, tile) * copies
            sums[box] = sums[box] + jnp.sum(product.reshape(16, 8, 128), axis=0)
    return sums


def solve(near_ref, inverse_ref, right_side, box):
    solved = row_of_sums(inverse_ref[box] * right_side)
    live = near_ref[2 * BOXES_HERE + box : 2 * BOXES_HERE + box + 1, :] > 0.5
    return jnp.where(live, solved, 0.0)


def far_of_all(samp_ref, parts_ref, rad_hbm, rad_ref, sems):
    for i in range(AHEAD_FAR):
        block_copy(rad_hbm, rad_ref, sems, i).start()
    samp_ref[...] = jnp.sum(parts_ref[...], axis=0)
    ones = jnp.ones((256, 128), BF16)

    def block(i, sums):
        first_line = pl.multiple_of(i * BLOCK, BLOCK)
        await_block(rad_hbm, rad_ref, sems, i, AHEAD_FAR)
        rad = lambda box, tile: rad_ref[
            box, pl.ds(pl.multiple_of(first_line + tile * 128, 128), 128), :
        ]
        return tuple(far_of_block(samp_ref, i * 8, rad, list(sums), ones))

    zero = jnp.zeros((8, 128), F32)
    return lax.fori_loop(0, STEPS_D, block, (zero,) * BOXES_HERE)


def first_step_kernel(
    parts_ref, near_ref, inverse_ref, second_ref, weight_ref, rad_hbm,
    current_ref, field_ref, rad_ref, samp_ref, dot_ref, sems,
):
    sums = far_of_all(samp_ref, parts_ref, rad_hbm, rad_ref, sems)
    ones = jnp.ones((256, 128), BF16)
    currents = []
    for box in range(BOXES_HERE):
        far = jnp.sum(sums[box], axis=0, keepdims=True)
        right_side = near_ref[box : box + 1, :] - far
        current = solve(near_ref, inverse_ref, right_side, box)
        current_ref[box : box + 1, :] = current
        currents.append(current)
    eye = identity_mask()

    def one_block(i, _):
        for tile in range(BLOCK // 128):
            start = pl.multiple_of(i * BLOCK + tile * 128, 128)
            product = rad_ref[0, pl.ds(start, 128), :] * currents[0]
            for box in range(1, BOXES_HERE):
                product = product + rad_ref[box, pl.ds(start, 128), :] * currents[box]
            high, low = split_two(product)
            copies_of = jnp.dot(
                jnp.concatenate([high, low], axis=1), ones, preferred_element_type=F32
            )
            dot_ref[tile : tile + 1, :] = jnp.sum(
                jnp.where(eye, copies_of, 0.0), axis=0, keepdims=True
            )
        response = dot_ref[...]
        rows = pl.ds(pl.multiple_of(i * 8, 8), 8)
        for target in range(CLUSTERS):
            field_ref[target, rows, :] = (
                second_ref[target, rows, :] + weight_ref[target, rows, :] * response
            )
        return 0

    lax.fori_loop(0, STEPS_D, one_block, 0)


def first_step(parts, near, self_inverse, second, weight, radiation):
    vmem = pl.BlockSpec(memory_space=VMEM)
    return pl.pallas_call(
        first_step_kernel,
        in_specs=[vmem] * 5 + [pl.BlockSpec(memory_space=pltpu.HBM)],
        out_specs=[vmem, vmem],
        out_shape=[
            jax.ShapeDtypeStruct((BOXES_HERE, PB), F32),
            jax.ShapeDtypeStruct((CLUSTERS, ROWS, 128), F32),
        ],
        scratch_shapes=[
            VMEM(radiation.shape, F32),
            VMEM((ROWS, 128), F32),
            VMEM((8, 128), F32),
            pltpu.SemaphoreType.DMA((STEPS_D,)),
        ],
        compiler_params=pltpu.CompilerParams(vmem_limit_bytes=28 << 20),
        cost_estimate=pl.CostEstimate(flops=4 << 30, bytes_accessed=20 << 20, transcendentals=0),
        name="first_step",
    )(parts, near, self_inverse, second, weight, in_hbm(radiation))


def second_step_kernel(
    parts_ref, near_ref, inverse_ref, before_ref, rad_hbm,
    out_ref, rad_ref, samp_ref, sems,
):
    sums = far_of_all(samp_ref, parts_ref, rad_hbm, rad_ref, sems)
    for box in range(BOXES_HERE):
        lanes = slice(box * PB, (box + 1) * PB)
        far = jnp.sum(sums[box], axis=0, keepdims=True)
        right_side = near_ref[box : box + 1, :] - far
        out_ref[0:1, lanes] = before_ref[box : box + 1, :]
        out_ref[1:2, lanes] = solve(near_ref, inverse_ref, right_side, box)


def second_step(parts, near, self_inverse, before, radiation):
    vmem = pl.BlockSpec(memory_space=VMEM)
    return pl.pallas_call(
        second_step_kernel,
        in_specs=[vmem] * 4 + [pl.BlockSpec(memory_space=pltpu.HBM)],
        out_specs=vmem,
        out_shape=jax.ShapeDtypeStruct((STEPS, BOXES_HERE * PB), F32),
        scratch_shapes=[
            VMEM(radiation.shape, F32),
            VMEM((ROWS, 128), F32),
            pltpu.SemaphoreType.DMA((STEPS_D,)),
        ],
        compiler_params=pltpu.CompilerParams(vmem_limit_bytes=28 << 20),
        cost_estimate=pl.CostEstimate(flops=4 << 30, bytes_accessed=20 << 20, transcendentals=0),
        name="second_step",
    )(parts, near, self_inverse, before, in_hbm(radiation))


def from_behind(array, by):
    axis = ("space", "ray")
    size = lax.axis_size(axis)
    pairs = [(i, i + by) for i in range(size) if 0 <= i + by < size]
    return lax.ppermute(array, axis, pairs)


def sum_kernel(arrived_ref, copies_ref):
    total = jnp.sum(arrived_ref[...], axis=0)
    for copy in range(copies_ref.shape[0]):
        copies_ref[copy] = total


def summed_copies(arrived, copies):
    vmem = pl.BlockSpec(memory_space=VMEM)
    return pl.pallas_call(
        sum_kernel,
        in_specs=[vmem],
        out_specs=vmem,
        out_shape=jax.ShapeDtypeStruct((copies, *arrived.shape[1:]), F32),
        compiler_params=pltpu.CompilerParams(vmem_limit_bytes=4 << 20),
        cost_estimate=pl.CostEstimate(flops=1 << 17, bytes_accessed=1 << 20, transcendentals=0),
        name="summed_copies",
    )(arrived)


def over_clusters(field):
    return lax.all_to_all(field, "space", split_axis=0, concat_axis=0, tiled=True)


def over_rays(copies):
    return lax.all_to_all(copies, "ray", split_axis=0, concat_axis=0, tiled=True)


def steps(
    excite, history, near_mats, neighbours, self_inverse, radiation, directions, centers, counts
):
    space = lax.axis_index("space").astype(jnp.int32).reshape(1)
    first_box = (lax.axis_index(("space", "ray")) * BOXES_HERE).astype(jnp.int32).reshape(1)
    ray_size = lax.axis_size("ray")
    first, out, twice, scale, recent = translate(space, centers, history, directions, radiation)
    upper = from_behind(recent, -1)
    second, weight = known_part(space, out, twice, scale)
    copies = summed_copies(over_clusters(first), ray_size)
    copies, upper, second, weight, recent = lax.optimization_barrier(
        (copies, upper, second, weight, recent)
    )
    parts = over_rays(copies)
    lower = from_behind(recent, 1)
    near = near_fields(
        first_box, neighbours, counts, excite, lower, recent, upper, near_mats
    )
    current, field = first_step(parts, near, self_inverse, second, weight, radiation)
    lower, upper = from_behind(current, 1), from_behind(current, -1)
    copies = summed_copies(over_clusters(field), ray_size)
    copies, lower, upper = lax.optimization_barrier((copies, lower, upper))
    parts = over_rays(copies)
    near = near_again(first_box, neighbours, lower, current, upper, near, near_mats)
    return second_step(parts, near, self_inverse, current, radiation)


def solution(mesh):
    placed = (
        P(None, ("space", "ray")),
        P(None, ("space", "ray")),
        P(("space", "ray"), None, None, None, None),
        P(("space", "ray"), None),
        P(("space", "ray"), None, None),
        P(("space", "ray"), None, None),
        P(),
        P(),
        P(("space", "ray")),
    )
    return jax.shard_map(
        steps, mesh=mesh, in_specs=placed, out_specs=P(None, ("space", "ray")), check_vma=False
    )
```

```python
import math

import jax
import jax.numpy as jnp
import numpy as np
from jax import lax
from jax.experimental import pallas as pl
from jax.experimental.pallas import tpu as pltpu
from jax.sharding import PartitionSpec as P


PB = 128
K = 64
TAU = 48
KN = 3
STEPS = 2
NB = 8
BOXES_HERE = 4
CLUSTERS = 16
FAR_TARGETS = 14
RAYS = 8192
ROWS = RAYS // 128
LINE = ROWS + 8
BLOCK = 1024
STEPS_D = RAYS // BLOCK
AHEAD = 2
AHEAD_FAR = 8
REACH = 2.0 * CLUSTERS + 4.0
VMEM = pltpu.VMEM
F32 = jnp.float32
BF16 = jnp.bfloat16


def basis_table():
    m = np.arange(TAU)[:, None] + 0.5
    k = np.arange(K)[None, :] + 0.5
    return np.sqrt(2.0 / K) * np.cos(np.pi * m * k / K)


def projection_table():
    basis = basis_table()
    table = np.zeros((128, K))
    table[:TAU] = basis
    table[TAU : 2 * TAU, : K - 1] = basis[:, 1:]
    return table.astype(np.float32)


def split_two(x):
    high = x.astype(BF16)
    return high, (x - high.astype(F32)).astype(BF16)


def identity_mask():
    return lax.broadcasted_iota(jnp.int32, (128, 128), 0) == lax.broadcasted_iota(
        jnp.int32, (128, 128), 1
    )


def row_of_sums(matrix):
    return jnp.sum(matrix.T, axis=0, keepdims=True)


def targets_of(me, centers_ref, dirs, target):
    dx, dy, dz = dirs
    sx = centers_ref[0, target] - centers_ref[0, me]
    sy = centers_ref[1, target] - centers_ref[1, me]
    sz = centers_ref[2, target] - centers_ref[2, me]
    squared = jnp.full((8, 128), sx * sx + sy * sy + sz * sz, F32)
    distant = jnp.abs(target - me) >= 2
    inverse = 1.0 / jnp.sqrt(jnp.where(distant, squared, 1.0))
    along = dx * sx + dy * sy + dz * sz
    u = (math.pi / 128.0) * (0.5 + along * (24.0 / REACH))
    v = u * u
    sin = u * (1 + v * (-1 / 6 + v * (1 / 120 + v * (-1 / 5040 + v * (1 / 362880)))))
    cos = 1 + v * (-1 / 2 + v * (1 / 24 + v * (-1 / 720 + v * (1 / 40320))))
    gain = (1.0 + along * inverse) * inverse * (0.5 * math.sqrt(2.0 / K) / math.sqrt(2.0))
    return -4.0 * sin * cos, jnp.where(distant, gain * (cos - sin), 0.0)


def clenshaw(terms_of, prepared, parts):
    zero = jnp.zeros((8, 128), F32)
    ones = [[zero] * parts for _ in prepared]
    twos = [[zero] * parts for _ in prepared]
    for m in reversed(range(TAU)):
        terms = terms_of(m)
        for inner, (twice, _) in enumerate(prepared):
            for part in range(parts):
                new = (terms[part] - twos[inner][part]) + twice * ones[inner][part]
                twos[inner][part] = ones[inner][part]
                ones[inner][part] = new
    return [
        [scale * (one - two) for one, two in zip(ones[inner], twos[inner])]
        for inner, (_, scale) in enumerate(prepared)
    ]


def block_rows(first, size):
    return pl.ds(first if isinstance(first, int) else pl.multiple_of(first, size), size)


def block_copy(rad_hbm, rad_ref, sems, i):
    lines = block_rows(i * BLOCK, BLOCK)
    return pltpu.make_async_copy(rad_hbm.at[:, lines, :], rad_ref.at[:, lines, :], sems.at[i])


def await_block(rad_hbm, rad_ref, sems, i, ahead):
    def start():
        block_copy(rad_hbm, rad_ref, sems, i + ahead).start()

    if isinstance(i, int):
        if i + ahead < STEPS_D:
            start()
    else:
        pl.when(i + ahead < STEPS_D)(start)
    block_copy(rad_hbm, rad_ref, sems, i).wait()


def translate_kernel(
    space_ref, centers_ref, table_hbm, history_hbm, dirs_hbm, rad_hbm,
    first_ref, second_ref, twice_ref, scale_ref, recent_ref,
    rad_ref, table_ref, history_ref, dirs_ref, lines_ref, proj_ref, out_ref, odd_ref, small_sems, sems,
):
    me = space_ref[0]
    start = jnp.where(me == CLUSTERS - 1, me + 1, me + 2)
    small = [
        pltpu.make_async_copy(source, target, small_sems.at[i])
        for i, (source, target) in enumerate(
            ((table_hbm, table_ref), (history_hbm, history_ref), (dirs_hbm, dirs_ref))
        )
    ]
    for copy in small:
        copy.start()
    for i in range(AHEAD):
        block_copy(rad_hbm, rad_ref, sems, i).start()
    for copy in small:
        copy.wait()
    recent_ref[...] = history_ref[0:8, :]
    for axis in range(3):
        for row in range(ROWS):
            lines_ref[axis * ROWS + row : axis * ROWS + row + 1, :] = dirs_ref[
                axis : axis + 1, row * 128 : (row + 1) * 128
            ]
    projected = jnp.dot(
        table_ref[...], history_ref[...], precision=lax.Precision.HIGHEST,
        preferred_element_type=F32,
    )
    for box in range(BOXES_HERE):
        high, low = split_two(projected[:, box * PB : (box + 1) * PB].T)
        proj_ref[box * PB : (box + 1) * PB, 0:128] = high
        proj_ref[box * PB : (box + 1) * PB, 128:256] = low
        proj_ref[(box + 4) * PB : (box + 5) * PB, 0:128] = high
        proj_ref[(box + 4) * PB : (box + 5) * PB, 128:256] = jnp.zeros((PB, 128), BF16)

    def project(i, quarter, slot):
        lines = block_rows(i * BLOCK + quarter * 256, 256)
        splits = [split_two(rad_ref[box, lines, :]) for box in range(BOXES_HERE)]
        pieces = jnp.concatenate([high for high, _ in splits] + [low for _, low in splits], axis=1)
        both = jnp.dot(pieces, proj_ref[...], preferred_element_type=F32)
        total = both[:, :128] + both[:, 128:]
        for inner in range(2):
            turned = total[inner * 128 : (inner + 1) * 128, :].T
            tile = quarter * 2 + inner
            for group in range(TAU // 8):
                slot[pl.ds(group * 8 * 9 + tile, 8, stride=9), :] = turned[
                    group * 8 : (group + 1) * 8, :
                ]
                place = pl.ds(group * 8 * LINE + i * 8 + tile, 8, stride=LINE)
                second_ref[place, :] = turned[TAU + group * 8 : TAU + (group + 1) * 8, :]

    def spread(i, quarter, slot):
        rows = block_rows(i * 8, 8)
        dirs = [lines_ref[block_rows(axis * ROWS + i * 8, 8), :] for axis in range(3)]
        places = range(quarter * 4, min(quarter * 4 + 4, FAR_TARGETS))
        targets = [lax.rem(start + place, CLUSTERS) for place in places]
        prepared = [targets_of(me, centers_ref, dirs, target) for target in targets]
        terms_of = lambda m: (slot[m * 9 : m * 9 + 8, :],)
        for target, result in zip(targets, clenshaw(terms_of, prepared, 1)):
            first_ref[target, rows, :] = result[0]
        for place, (twice, scale) in zip(places, prepared):
            twice_ref[place, rows, :] = twice
            scale_ref[place, rows, :] = scale
        if quarter == 3:
            for inner in range(FAR_TARGETS, CLUSTERS):
                first_ref[lax.rem(start + inner, CLUSTERS), rows, :] = jnp.zeros((8, 128), F32)

    def both_of(i, slot, before):
        await_block(rad_hbm, rad_ref, sems, i, AHEAD)
        for quarter in range(4):
            project(i, quarter, slot)
            spread(i - 1, quarter, before)

    def two_blocks(pair, _):
        both_of(2 * pair + 1, odd_ref, out_ref)
        both_of(2 * pair + 2, out_ref, odd_ref)
        return 0

    await_block(rad_hbm, rad_ref, sems, 0, AHEAD)
    for quarter in range(4):
        project(0, quarter, out_ref)
    lax.fori_loop(0, STEPS_D // 2 - 1, two_blocks, 0)
    both_of(STEPS_D - 1, odd_ref, out_ref)
    for quarter in range(4):
        spread(STEPS_D - 1, quarter, odd_ref)


def in_hbm(x):
    return pltpu.with_memory_space_constraint(x, pltpu.HBM)


def translate(space, centers, history, dirs, radiation):
    smem = pl.BlockSpec(memory_space=pltpu.SMEM)
    hbm = pl.BlockSpec(memory_space=pltpu.HBM)
    vmem = pl.BlockSpec(memory_space=VMEM)
    table = jnp.asarray(projection_table())
    return pl.pallas_call(
        translate_kernel,
        in_specs=[smem, smem, hbm, hbm, hbm, hbm],
        out_specs=[vmem] * 5,
        out_shape=[
            jax.ShapeDtypeStruct((CLUSTERS, ROWS, 128), F32),
            jax.ShapeDtypeStruct((TAU * LINE, 128), F32),
            pltpu.HBM((FAR_TARGETS, ROWS, 128), F32),
            pltpu.HBM((FAR_TARGETS, ROWS, 128), F32),
            jax.ShapeDtypeStruct((8, history.shape[1]), F32),
        ],
        scratch_shapes=[
            VMEM(radiation.shape, F32),
            VMEM((128, K), F32),
            VMEM(history.shape, F32),
            VMEM(dirs.shape, F32),
            VMEM((3 * ROWS, 128), F32),
            VMEM((8 * PB, 256), BF16),
            VMEM((TAU * 9, 128), F32),
            VMEM((TAU * 9, 128), F32),
            pltpu.SemaphoreType.DMA((3,)),
            pltpu.SemaphoreType.DMA((STEPS_D,)),
        ],
        compiler_params=pltpu.CompilerParams(vmem_limit_bytes=28 << 20),
        cost_estimate=pl.CostEstimate(flops=8 << 30, bytes_accessed=20 << 20, transcendentals=0),
        name="translate",
    )(space, in_hbm(centers), in_hbm(table), in_hbm(history), in_hbm(dirs), in_hbm(radiation))


def newest_weight(twice, scale):
    c = 0.5 * twice
    squared = c * c
    s = jnp.sqrt(1.0 - squared)
    half_sin = jnp.sqrt(0.5 - 0.5 * c)
    half_cos = jnp.sqrt(0.5 + 0.5 * c)
    c, s = c * (4.0 * squared - 3.0), s * (4.0 * squared - 1.0)
    for _ in range(4):
        c, s = 1.0 - 2.0 * (s * s), 2.0 * (s * c)
    shift, small = 48.0 * math.pi / 128.0, math.pi / 256.0
    total = (s * math.cos(shift) + c * math.sin(shift)) / (
        half_sin * math.cos(small) + half_cos * math.sin(small)
    ) + (s * math.cos(shift) - c * math.sin(shift)) / (
        half_sin * math.cos(small) - half_cos * math.sin(small)
    )
    return (0.25 * math.sqrt(2.0 / K)) * scale * total / half_cos


def known_kernel(space_ref, out_ref, twice_ref, scale_ref, second_ref, weight_ref):
    me = space_ref[0]
    start = jnp.where(me == CLUSTERS - 1, me + 1, me + 2)

    def block(i, _):
        rows = pl.ds(pl.multiple_of(i * 8, 8), 8)
        terms_of = lambda m: (out_ref[pl.ds(pl.multiple_of(m * LINE + i * 8, 8), 8), :],)

        def targets_group(group, _):
            first = group * 7
            prepared = [
                (twice_ref[first + inner, rows, :], scale_ref[first + inner, rows, :])
                for inner in range(7)
            ]
            for inner, result in enumerate(clenshaw(terms_of, prepared, 1)):
                target = lax.rem(start + first + inner, CLUSTERS)
                second_ref[target, rows, :] = result[0]
                weight_ref[target, rows, :] = newest_weight(*prepared[inner])
            return 0

        lax.fori_loop(0, FAR_TARGETS // 7, targets_group, 0)
        for inner in range(FAR_TARGETS, CLUSTERS):
            target = lax.rem(start + inner, CLUSTERS)
            second_ref[target, rows, :] = jnp.zeros((8, 128), F32)
            weight_ref[target, rows, :] = jnp.zeros((8, 128), F32)
        return 0

    lax.fori_loop(0, STEPS_D, block, 0)


def known_part(space, out, twice, scale):
    smem = pl.BlockSpec(memory_space=pltpu.SMEM)
    vmem = pl.BlockSpec(memory_space=VMEM)
    shape = pltpu.HBM((CLUSTERS, ROWS, 128), F32)
    return pl.pallas_call(
        known_kernel,
        in_specs=[smem, vmem, vmem, vmem],
        out_specs=[vmem, vmem],
        out_shape=[shape, shape],
        compiler_params=pltpu.CompilerParams(vmem_limit_bytes=8 << 20),
        cost_estimate=pl.CostEstimate(flops=20 << 20, bytes_accessed=4 << 20, transcendentals=0),
        name="known_part",
    )(space, out, in_hbm(twice), in_hbm(scale))


def near_kernel(
    first_box_ref, nb_ref, counts_ref, excite_ref, lower_ref, own_ref, upper_ref, mats_hbm,
    out_ref, mats_ref, win_ref, sems,
):
    def copy_of(box):
        return pltpu.make_async_copy(mats_hbm.at[box], mats_ref.at[box], sems.at[box])

    for box in range(BOXES_HERE):
        copy_of(box).start()
    for k in range(KN):
        for place, ref in enumerate((lower_ref, own_ref, upper_ref)):
            for inner in range(BOXES_HERE):
                row = (place * BOXES_HERE + inner) * 8 + k
                win_ref[row : row + 1, :] = ref[k : k + 1, inner * PB : (inner + 1) * PB]
    for step in range(STEPS):
        for box in range(BOXES_HERE):
            row = step * BOXES_HERE + box
            out_ref[row : row + 1, :] = excite_ref[step : step + 1, box * PB : (box + 1) * PB]

    def one_box(box, _):
        copy_of(box).wait()
        first = jnp.zeros((128, 128), F32)
        second = jnp.zeros((128, 128), F32)
        for j in range(NB):
            place = (nb_ref[box, j] - first_box_ref[0] + BOXES_HERE) * 8
            rows = [win_ref[pl.ds(place + k, 1), :] for k in range(KN)]
            for k in range(KN):
                mats = mats_ref[box, j, k]
                first = first + mats * rows[k]
                if k:
                    second = second + mats * rows[k - 1]
        for step, total in enumerate((first, second)):
            row = pl.ds(box + step * BOXES_HERE, 1)
            out_ref[row, :] = out_ref[row, :] - row_of_sums(total)
        live = lax.broadcasted_iota(jnp.int32, (1, PB), 1) < counts_ref[box]
        out_ref[pl.ds(box + 2 * BOXES_HERE, 1), :] = jnp.where(live, 1.0, 0.0)
        return 0

    lax.fori_loop(0, BOXES_HERE, one_box, 0)


def near_fields(first_box, neighbours, counts, excite, lower, recent, upper, near_mats):
    smem = pl.BlockSpec(memory_space=pltpu.SMEM)
    vmem = pl.BlockSpec(memory_space=VMEM)
    return pl.pallas_call(
        near_kernel,
        in_specs=[smem] * 3 + [vmem] * 4 + [pl.BlockSpec(memory_space=pltpu.HBM)],
        out_specs=vmem,
        out_shape=jax.ShapeDtypeStruct((16, PB), F32),
        scratch_shapes=[
            VMEM(near_mats.shape, F32),
            VMEM((3 * BOXES_HERE * 8, PB), F32),
            pltpu.SemaphoreType.DMA((BOXES_HERE,)),
        ],
        compiler_params=pltpu.CompilerParams(vmem_limit_bytes=9 << 20),
        cost_estimate=pl.CostEstimate(flops=1 << 30, bytes_accessed=7 << 20, transcendentals=0),
        name="near_fields",
    )(first_box, neighbours, counts, excite, lower, recent, upper, in_hbm(near_mats))


def near_again_kernel(
    first_box_ref, nb_ref, lower_ref, own_ref, upper_ref, before_ref, mats_ref, out_ref, win_ref
):
    box = pl.program_id(0)

    @pl.when(box == 0)
    def _():
        for place, ref in enumerate((lower_ref, own_ref, upper_ref)):
            win_ref[place * BOXES_HERE : (place + 1) * BOXES_HERE, :] = ref[...]

    total = jnp.zeros((128, 128), F32)
    for j in range(NB):
        place = nb_ref[box, j] - first_box_ref[0] + BOXES_HERE
        total = total + mats_ref[0, j, 0] * win_ref[pl.ds(place, 1), :]
    out_ref[pl.ds(box, 1), :] = before_ref[pl.ds(box + BOXES_HERE, 1), :] - row_of_sums(total)
    out_ref[pl.ds(box + 2 * BOXES_HERE, 1), :] = before_ref[pl.ds(box + 2 * BOXES_HERE, 1), :]


def near_again(first_box, neighbours, lower, own, upper, before, near_mats):
    smem = pl.BlockSpec(memory_space=pltpu.SMEM)
    side = pl.BlockSpec((BOXES_HERE, PB), lambda i: (0, 0))
    return pl.pallas_call(
        near_again_kernel,
        grid=(BOXES_HERE,),
        in_specs=[
            smem,
            smem,
            side,
            side,
            side,
            pl.BlockSpec((16, PB), lambda i: (0, 0)),
            pl.BlockSpec((1, NB, 1, PB, PB), lambda i: (i, 0, 0, 0, 0)),
        ],
        out_specs=pl.BlockSpec((16, PB), lambda i: (0, 0)),
        out_shape=jax.ShapeDtypeStruct((16, PB), F32),
        scratch_shapes=[VMEM((16, PB), F32)],
        compiler_params=pltpu.CompilerParams(vmem_limit_bytes=6 << 20),
        cost_estimate=pl.CostEstimate(flops=1 << 29, bytes_accessed=3 << 20, transcendentals=0),
        name="near_again",
    )(first_box, neighbours, lower, own, upper, before, in_hbm(near_mats))


def far_of_block(samp_ref, rows, rad, sums, ones):
    eye = identity_mask()
    for tile in range(BLOCK // 128):
        row = samp_ref[pl.ds(rows + tile, 1), :]
        high = row.astype(BF16).astype(F32)
        low = row - high
        spread = jnp.concatenate(
            [jnp.where(eye, high, 0.0).astype(BF16), jnp.where(eye, low, 0.0).astype(BF16)], axis=1
        )
        copies = jnp.dot(spread, ones, preferred_element_type=F32)
        for box in range(BOXES_HERE):
            product = rad(box, tile) * copies
            sums[box] = sums[box] + jnp.sum(product.reshape(16, 8, 128), axis=0)
    return sums


def solve(near_ref, inverse_ref, right_side, box):
    solved = row_of_sums(inverse_ref[box] * right_side)
    live = near_ref[2 * BOXES_HERE + box : 2 * BOXES_HERE + box + 1, :] > 0.5
    return jnp.where(live, solved, 0.0)


def far_of_all(samp_ref, parts_ref, rad_hbm, rad_ref, sems):
    for i in range(AHEAD_FAR):
        block_copy(rad_hbm, rad_ref, sems, i).start()
    samp_ref[...] = jnp.sum(parts_ref[...], axis=0)
    ones = jnp.ones((256, 128), BF16)

    def block(i, sums):
        first_line = pl.multiple_of(i * BLOCK, BLOCK)
        await_block(rad_hbm, rad_ref, sems, i, AHEAD_FAR)
        rad = lambda box, tile: rad_ref[
            box, pl.ds(pl.multiple_of(first_line + tile * 128, 128), 128), :
        ]
        return tuple(far_of_block(samp_ref, i * 8, rad, list(sums), ones))

    zero = jnp.zeros((8, 128), F32)
    return lax.fori_loop(0, STEPS_D, block, (zero,) * BOXES_HERE)


def first_step_kernel(
    parts_ref, near_ref, inverse_ref, second_ref, weight_ref, rad_hbm,
    current_ref, field_ref, rad_ref, samp_ref, dot_ref, sems,
):
    sums = far_of_all(samp_ref, parts_ref, rad_hbm, rad_ref, sems)
    ones = jnp.ones((256, 128), BF16)
    currents = []
    for box in range(BOXES_HERE):
        far = jnp.sum(sums[box], axis=0, keepdims=True)
        right_side = near_ref[box : box + 1, :] - far
        current = solve(near_ref, inverse_ref, right_side, box)
        current_ref[box : box + 1, :] = current
        currents.append(current)
    eye = identity_mask()

    def one_block(i, _):
        for tile in range(BLOCK // 128):
            start = pl.multiple_of(i * BLOCK + tile * 128, 128)
            product = rad_ref[0, pl.ds(start, 128), :] * currents[0]
            for box in range(1, BOXES_HERE):
                product = product + rad_ref[box, pl.ds(start, 128), :] * currents[box]
            high, low = split_two(product)
            copies_of = jnp.dot(
                jnp.concatenate([high, low], axis=1), ones, preferred_element_type=F32
            )
            dot_ref[tile : tile + 1, :] = jnp.sum(
                jnp.where(eye, copies_of, 0.0), axis=0, keepdims=True
            )
        response = dot_ref[...]
        rows = pl.ds(pl.multiple_of(i * 8, 8), 8)
        for target in range(CLUSTERS):
            field_ref[target, rows, :] = (
                second_ref[target, rows, :] + weight_ref[target, rows, :] * response
            )
        return 0

    lax.fori_loop(0, STEPS_D, one_block, 0)


def first_step(parts, near, self_inverse, second, weight, radiation):
    vmem = pl.BlockSpec(memory_space=VMEM)
    return pl.pallas_call(
        first_step_kernel,
        in_specs=[vmem] * 5 + [pl.BlockSpec(memory_space=pltpu.HBM)],
        out_specs=[vmem, vmem],
        out_shape=[
            jax.ShapeDtypeStruct((BOXES_HERE, PB), F32),
            jax.ShapeDtypeStruct((CLUSTERS, ROWS, 128), F32),
        ],
        scratch_shapes=[
            VMEM(radiation.shape, F32),
            VMEM((ROWS, 128), F32),
            VMEM((8, 128), F32),
            pltpu.SemaphoreType.DMA((STEPS_D,)),
        ],
        compiler_params=pltpu.CompilerParams(vmem_limit_bytes=28 << 20),
        cost_estimate=pl.CostEstimate(flops=4 << 30, bytes_accessed=20 << 20, transcendentals=0),
        name="first_step",
    )(parts, near, self_inverse, second, weight, in_hbm(radiation))


def second_step_kernel(
    parts_ref, near_ref, inverse_ref, before_ref, rad_hbm,
    out_ref, rad_ref, samp_ref, sems,
):
    sums = far_of_all(samp_ref, parts_ref, rad_hbm, rad_ref, sems)
    for box in range(BOXES_HERE):
        lanes = slice(box * PB, (box + 1) * PB)
        far = jnp.sum(sums[box], axis=0, keepdims=True)
        right_side = near_ref[box : box + 1, :] - far
        out_ref[0:1, lanes] = before_ref[box : box + 1, :]
        out_ref[1:2, lanes] = solve(near_ref, inverse_ref, right_side, box)


def second_step(parts, near, self_inverse, before, radiation):
    vmem = pl.BlockSpec(memory_space=VMEM)
    return pl.pallas_call(
        second_step_kernel,
        in_specs=[vmem] * 4 + [pl.BlockSpec(memory_space=pltpu.HBM)],
        out_specs=vmem,
        out_shape=jax.ShapeDtypeStruct((STEPS, BOXES_HERE * PB), F32),
        scratch_shapes=[
            VMEM(radiation.shape, F32),
            VMEM((ROWS, 128), F32),
            pltpu.SemaphoreType.DMA((STEPS_D,)),
        ],
        compiler_params=pltpu.CompilerParams(vmem_limit_bytes=28 << 20),
        cost_estimate=pl.CostEstimate(flops=4 << 30, bytes_accessed=20 << 20, transcendentals=0),
        name="second_step",
    )(parts, near, self_inverse, before, in_hbm(radiation))


def from_behind(array, by):
    axis = ("space", "ray")
    size = lax.axis_size(axis)
    pairs = [(i, i + by) for i in range(size) if 0 <= i + by < size]
    return lax.ppermute(array, axis, pairs)


def sum_kernel(arrived_ref, copies_ref):
    total = jnp.sum(arrived_ref[...], axis=0)
    for copy in range(copies_ref.shape[0]):
        copies_ref[copy] = total


def summed_copies(arrived, copies):
    vmem = pl.BlockSpec(memory_space=VMEM)
    return pl.pallas_call(
        sum_kernel,
        in_specs=[vmem],
        out_specs=vmem,
        out_shape=jax.ShapeDtypeStruct((copies, *arrived.shape[1:]), F32),
        compiler_params=pltpu.CompilerParams(vmem_limit_bytes=4 << 20),
        cost_estimate=pl.CostEstimate(flops=1 << 17, bytes_accessed=1 << 20, transcendentals=0),
        name="summed_copies",
    )(arrived)


def over_clusters(field):
    return lax.all_to_all(field, "space", split_axis=0, concat_axis=0, tiled=True)


def over_rays(copies):
    return lax.all_to_all(copies, "ray", split_axis=0, concat_axis=0, tiled=True)


def steps(
    excite, history, near_mats, neighbours, self_inverse, radiation, directions, centers, counts
):
    space = lax.axis_index("space").astype(jnp.int32).reshape(1)
    first_box = (lax.axis_index(("space", "ray")) * BOXES_HERE).astype(jnp.int32).reshape(1)
    ray_size = lax.axis_size("ray")
    first, out, twice, scale, recent = translate(space, centers, history, directions, radiation)
    upper = from_behind(recent, -1)
    second, weight = known_part(space, out, twice, scale)
    copies = summed_copies(over_clusters(first), ray_size)
    copies, upper, second, weight, recent = lax.optimization_barrier(
        (copies, upper, second, weight, recent)
    )
    parts = over_rays(copies)
    lower = from_behind(recent, 1)
    near = near_fields(
        first_box, neighbours, counts, excite, lower, recent, upper, near_mats
    )
    current, field = first_step(parts, near, self_inverse, second, weight, radiation)
    lower, upper = from_behind(current, 1), from_behind(current, -1)
    copies = summed_copies(over_clusters(field), ray_size)
    copies, lower, upper = lax.optimization_barrier((copies, lower, upper))
    parts = over_rays(copies)
    near = near_again(first_box, neighbours, lower, current, upper, near, near_mats)
    return second_step(parts, near, self_inverse, current, radiation)


def solution(mesh):
    placed = (
        P(None, ("space", "ray")),
        P(None, ("space", "ray")),
        P(("space", "ray"), None, None, None, None),
        P(("space", "ray"), None),
        P(("space", "ray"), None, None),
        P(("space", "ray"), None, None),
        P(),
        P(),
        P(("space", "ray")),
    )
    return jax.shard_map(
        steps, mesh=mesh, in_specs=placed, out_specs=P(None, ("space", "ray")), check_vma=False
    )
```

```python
import math

import jax
import jax.numpy as jnp
import numpy as np
from jax import lax
from jax.experimental import pallas as pl
from jax.experimental.pallas import tpu as pltpu
from jax.sharding import PartitionSpec as P


PB = 128
K = 64
TAU = 48
KN = 3
STEPS = 2
NB = 8
BOXES_HERE = 4
CLUSTERS = 16
FAR_TARGETS = 14
RAYS = 8192
ROWS = RAYS // 128
LINE = ROWS + 8
BLOCK = 1024
STEPS_D = RAYS // BLOCK
AHEAD = 2
AHEAD_FAR = 8
REACH = 2.0 * CLUSTERS + 4.0
VMEM = pltpu.VMEM
F32 = jnp.float32
BF16 = jnp.bfloat16


def basis_table():
    m = np.arange(TAU)[:, None] + 0.5
    k = np.arange(K)[None, :] + 0.5
    return np.sqrt(2.0 / K) * np.cos(np.pi * m * k / K)


def projection_table():
    basis = basis_table()
    table = np.zeros((128, K))
    table[:TAU] = basis
    table[TAU : 2 * TAU, : K - 1] = basis[:, 1:]
    return table.astype(np.float32)


def split_two(x):
    high = x.astype(BF16)
    return high, (x - high.astype(F32)).astype(BF16)


def identity_mask():
    return lax.broadcasted_iota(jnp.int32, (128, 128), 0) == lax.broadcasted_iota(
        jnp.int32, (128, 128), 1
    )


def row_of_sums(matrix):
    return jnp.sum(matrix.T, axis=0, keepdims=True)


def targets_of(me, centers_ref, dirs, target):
    dx, dy, dz = dirs
    sx = centers_ref[0, target] - centers_ref[0, me]
    sy = centers_ref[1, target] - centers_ref[1, me]
    sz = centers_ref[2, target] - centers_ref[2, me]
    squared = jnp.full((8, 128), sx * sx + sy * sy + sz * sz, F32)
    distant = jnp.abs(target - me) >= 2
    inverse = 1.0 / jnp.sqrt(jnp.where(distant, squared, 1.0))
    along = dx * sx + dy * sy + dz * sz
    u = (math.pi / 128.0) * (0.5 + along * (24.0 / REACH))
    v = u * u
    sin = u * (1 + v * (-1 / 6 + v * (1 / 120 + v * (-1 / 5040 + v * (1 / 362880)))))
    cos = 1 + v * (-1 / 2 + v * (1 / 24 + v * (-1 / 720 + v * (1 / 40320))))
    gain = (1.0 + along * inverse) * inverse * (0.5 * math.sqrt(2.0 / K) / math.sqrt(2.0))
    return -4.0 * sin * cos, jnp.where(distant, gain * (cos - sin), 0.0)


def clenshaw(terms_of, prepared, parts):
    zero = jnp.zeros((8, 128), F32)
    ones = [[zero] * parts for _ in prepared]
    twos = [[zero] * parts for _ in prepared]
    for m in reversed(range(TAU)):
        terms = terms_of(m)
        for inner, (twice, _) in enumerate(prepared):
            for part in range(parts):
                new = (terms[part] - twos[inner][part]) + twice * ones[inner][part]
                twos[inner][part] = ones[inner][part]
                ones[inner][part] = new
    return [
        [scale * (one - two) for one, two in zip(ones[inner], twos[inner])]
        for inner, (_, scale) in enumerate(prepared)
    ]


def block_rows(first, size):
    return pl.ds(first if isinstance(first, int) else pl.multiple_of(first, size), size)


def block_copy(rad_hbm, rad_ref, sems, i):
    lines = block_rows(i * BLOCK, BLOCK)
    return pltpu.make_async_copy(rad_hbm.at[:, lines, :], rad_ref.at[:, lines, :], sems.at[i])


def await_block(rad_hbm, rad_ref, sems, i, ahead):
    def start():
        block_copy(rad_hbm, rad_ref, sems, i + ahead).start()

    if isinstance(i, int):
        if i + ahead < STEPS_D:
            start()
    else:
        pl.when(i + ahead < STEPS_D)(start)
    block_copy(rad_hbm, rad_ref, sems, i).wait()


def translate_kernel(
    space_ref, centers_ref, table_hbm, history_hbm, dirs_hbm, rad_hbm,
    first_ref, second_ref, twice_ref, scale_ref, recent_ref,
    rad_ref, table_ref, history_ref, dirs_ref, lines_ref, proj_ref, out_ref, odd_ref, small_sems, sems,
):
    me = space_ref[0]
    start = jnp.where(me == CLUSTERS - 1, me + 1, me + 2)
    small = [
        pltpu.make_async_copy(source, target, small_sems.at[i])
        for i, (source, target) in enumerate(
            ((table_hbm, table_ref), (history_hbm, history_ref), (dirs_hbm, dirs_ref))
        )
    ]
    for copy in small:
        copy.start()
    for i in range(AHEAD):
        block_copy(rad_hbm, rad_ref, sems, i).start()
    for copy in small:
        copy.wait()
    recent_ref[...] = history_ref[0:8, :]
    for axis in range(3):
        for row in range(ROWS):
            lines_ref[axis * ROWS + row : axis * ROWS + row + 1, :] = dirs_ref[
                axis : axis + 1, row * 128 : (row + 1) * 128
            ]
    projected = jnp.dot(
        table_ref[...], history_ref[...], precision=lax.Precision.HIGHEST,
        preferred_element_type=F32,
    )
    for box in range(BOXES_HERE):
        high, low = split_two(projected[:, box * PB : (box + 1) * PB].T)
        proj_ref[box * PB : (box + 1) * PB, 0:128] = high
        proj_ref[box * PB : (box + 1) * PB, 128:256] = low
        proj_ref[(box + 4) * PB : (box + 5) * PB, 0:128] = high
        proj_ref[(box + 4) * PB : (box + 5) * PB, 128:256] = jnp.zeros((PB, 128), BF16)

    def project(i, quarter, slot):
        lines = block_rows(i * BLOCK + quarter * 256, 256)
        splits = [split_two(rad_ref[box, lines, :]) for box in range(BOXES_HERE)]
        pieces = jnp.concatenate([high for high, _ in splits] + [low for _, low in splits], axis=1)
        both = jnp.dot(pieces, proj_ref[...], preferred_element_type=F32)
        total = both[:, :128] + both[:, 128:]
        for inner in range(2):
            turned = total[inner * 128 : (inner + 1) * 128, :].T
            tile = quarter * 2 + inner
            for group in range(TAU // 8):
                slot[pl.ds(group * 8 * 9 + tile, 8, stride=9), :] = turned[
                    group * 8 : (group + 1) * 8, :
                ]
                place = pl.ds(group * 8 * LINE + i * 8 + tile, 8, stride=LINE)
                second_ref[place, :] = turned[TAU + group * 8 : TAU + (group + 1) * 8, :]

    def spread(i, quarter, slot):
        rows = block_rows(i * 8, 8)
        dirs = [lines_ref[block_rows(axis * ROWS + i * 8, 8), :] for axis in range(3)]
        places = range(quarter * 4, min(quarter * 4 + 4, FAR_TARGETS))
        targets = [lax.rem(start + place, CLUSTERS) for place in places]
        prepared = [targets_of(me, centers_ref, dirs, target) for target in targets]
        terms_of = lambda m: (slot[m * 9 : m * 9 + 8, :],)
        for target, result in zip(targets, clenshaw(terms_of, prepared, 1)):
            first_ref[target, rows, :] = result[0]
        for place, (twice, scale) in zip(places, prepared):
            twice_ref[place, rows, :] = twice
            scale_ref[place, rows, :] = scale
        if quarter == 3:
            for inner in range(FAR_TARGETS, CLUSTERS):
                first_ref[lax.rem(start + inner, CLUSTERS), rows, :] = jnp.zeros((8, 128), F32)

    def both_of(i, slot, before):
        await_block(rad_hbm, rad_ref, sems, i, AHEAD)
        for quarter in range(4):
            project(i, quarter, slot)
            spread(i - 1, quarter, before)

    def two_blocks(pair, _):
        both_of(2 * pair + 1, odd_ref, out_ref)
        both_of(2 * pair + 2, out_ref, odd_ref)
        return 0

    await_block(rad_hbm, rad_ref, sems, 0, AHEAD)
    for quarter in range(4):
        project(0, quarter, out_ref)
    lax.fori_loop(0, STEPS_D // 2 - 1, two_blocks, 0)
    both_of(STEPS_D - 1, odd_ref, out_ref)
    for quarter in range(4):
        spread(STEPS_D - 1, quarter, odd_ref)


def in_hbm(x):
    return pltpu.with_memory_space_constraint(x, pltpu.HBM)


def translate(space, centers, history, dirs, radiation):
    smem = pl.BlockSpec(memory_space=pltpu.SMEM)
    hbm = pl.BlockSpec(memory_space=pltpu.HBM)
    vmem = pl.BlockSpec(memory_space=VMEM)
    table = jnp.asarray(projection_table())
    return pl.pallas_call(
        translate_kernel,
        in_specs=[smem, smem, hbm, hbm, hbm, hbm],
        out_specs=[vmem] * 5,
        out_shape=[
            jax.ShapeDtypeStruct((CLUSTERS, ROWS, 128), F32),
            jax.ShapeDtypeStruct((TAU * LINE, 128), F32),
            pltpu.HBM((FAR_TARGETS, ROWS, 128), F32),
            pltpu.HBM((FAR_TARGETS, ROWS, 128), F32),
            jax.ShapeDtypeStruct((8, history.shape[1]), F32),
        ],
        scratch_shapes=[
            VMEM(radiation.shape, F32),
            VMEM((128, K), F32),
            VMEM(history.shape, F32),
            VMEM(dirs.shape, F32),
            VMEM((3 * ROWS, 128), F32),
            VMEM((8 * PB, 256), BF16),
            VMEM((TAU * 9, 128), F32),
            VMEM((TAU * 9, 128), F32),
            pltpu.SemaphoreType.DMA((3,)),
            pltpu.SemaphoreType.DMA((STEPS_D,)),
        ],
        compiler_params=pltpu.CompilerParams(vmem_limit_bytes=28 << 20),
        cost_estimate=pl.CostEstimate(flops=8 << 30, bytes_accessed=20 << 20, transcendentals=0),
        name="translate",
    )(space, in_hbm(centers), in_hbm(table), in_hbm(history), in_hbm(dirs), in_hbm(radiation))


def newest_weight(twice, scale):
    c = 0.5 * twice
    squared = c * c
    s = jnp.sqrt(1.0 - squared)
    half_sin = jnp.sqrt(0.5 - 0.5 * c)
    half_cos = jnp.sqrt(0.5 + 0.5 * c)
    c, s = c * (4.0 * squared - 3.0), s * (4.0 * squared - 1.0)
    for _ in range(4):
        c, s = 1.0 - 2.0 * (s * s), 2.0 * (s * c)
    shift, small = 48.0 * math.pi / 128.0, math.pi / 256.0
    total = (s * math.cos(shift) + c * math.sin(shift)) / (
        half_sin * math.cos(small) + half_cos * math.sin(small)
    ) + (s * math.cos(shift) - c * math.sin(shift)) / (
        half_sin * math.cos(small) - half_cos * math.sin(small)
    )
    return (0.25 * math.sqrt(2.0 / K)) * scale * total / half_cos


def known_kernel(space_ref, out_ref, twice_ref, scale_ref, second_ref, weight_ref):
    me = space_ref[0]
    start = jnp.where(me == CLUSTERS - 1, me + 1, me + 2)

    def block(i, _):
        rows = pl.ds(pl.multiple_of(i * 8, 8), 8)
        terms_of = lambda m: (out_ref[pl.ds(pl.multiple_of(m * LINE + i * 8, 8), 8), :],)

        def targets_group(group, _):
            first = group * 7
            prepared = [
                (twice_ref[first + inner, rows, :], scale_ref[first + inner, rows, :])
                for inner in range(7)
            ]
            for inner, result in enumerate(clenshaw(terms_of, prepared, 1)):
                target = lax.rem(start + first + inner, CLUSTERS)
                second_ref[target, rows, :] = result[0]
                weight_ref[target, rows, :] = newest_weight(*prepared[inner])
            return 0

        lax.fori_loop(0, FAR_TARGETS // 7, targets_group, 0)
        for inner in range(FAR_TARGETS, CLUSTERS):
            target = lax.rem(start + inner, CLUSTERS)
            second_ref[target, rows, :] = jnp.zeros((8, 128), F32)
            weight_ref[target, rows, :] = jnp.zeros((8, 128), F32)
        return 0

    lax.fori_loop(0, STEPS_D, block, 0)


def known_part(space, out, twice, scale):
    smem = pl.BlockSpec(memory_space=pltpu.SMEM)
    vmem = pl.BlockSpec(memory_space=VMEM)
    shape = pltpu.HBM((CLUSTERS, ROWS, 128), F32)
    return pl.pallas_call(
        known_kernel,
        in_specs=[smem, vmem, vmem, vmem],
        out_specs=[vmem, vmem],
        out_shape=[shape, shape],
        compiler_params=pltpu.CompilerParams(vmem_limit_bytes=8 << 20),
        cost_estimate=pl.CostEstimate(flops=20 << 20, bytes_accessed=4 << 20, transcendentals=0),
        name="known_part",
    )(space, out, in_hbm(twice), in_hbm(scale))


def near_kernel(
    first_box_ref, nb_ref, counts_ref, excite_ref, lower_ref, own_ref, upper_ref, mats_hbm,
    out_ref, mats_ref, win_ref, sems,
):
    def copy_of(box):
        return pltpu.make_async_copy(mats_hbm.at[box], mats_ref.at[box], sems.at[box])

    for box in range(BOXES_HERE):
        copy_of(box).start()
    for k in range(KN):
        for place, ref in enumerate((lower_ref, own_ref, upper_ref)):
            for inner in range(BOXES_HERE):
                row = (place * BOXES_HERE + inner) * 8 + k
                win_ref[row : row + 1, :] = ref[k : k + 1, inner * PB : (inner + 1) * PB]
    for step in range(STEPS):
        for box in range(BOXES_HERE):
            row = step * BOXES_HERE + box
            out_ref[row : row + 1, :] = excite_ref[step : step + 1, box * PB : (box + 1) * PB]

    def one_box(box, _):
        copy_of(box).wait()
        first = jnp.zeros((128, 128), F32)
        second = jnp.zeros((128, 128), F32)
        for j in range(NB):
            place = (nb_ref[box, j] - first_box_ref[0] + BOXES_HERE) * 8
            rows = [win_ref[pl.ds(place + k, 1), :] for k in range(KN)]
            for k in range(KN):
                mats = mats_ref[box, j, k]
                first = first + mats * rows[k]
                if k:
                    second = second + mats * rows[k - 1]
        for step, total in enumerate((first, second)):
            row = pl.ds(box + step * BOXES_HERE, 1)
            out_ref[row, :] = out_ref[row, :] - row_of_sums(total)
        live = lax.broadcasted_iota(jnp.int32, (1, PB), 1) < counts_ref[box]
        out_ref[pl.ds(box + 2 * BOXES_HERE, 1), :] = jnp.where(live, 1.0, 0.0)
        return 0

    lax.fori_loop(0, BOXES_HERE, one_box, 0)


def near_fields(first_box, neighbours, counts, excite, lower, recent, upper, near_mats):
    smem = pl.BlockSpec(memory_space=pltpu.SMEM)
    vmem = pl.BlockSpec(memory_space=VMEM)
    return pl.pallas_call(
        near_kernel,
        in_specs=[smem] * 3 + [vmem] * 4 + [pl.BlockSpec(memory_space=pltpu.HBM)],
        out_specs=vmem,
        out_shape=jax.ShapeDtypeStruct((16, PB), F32),
        scratch_shapes=[
            VMEM(near_mats.shape, F32),
            VMEM((3 * BOXES_HERE * 8, PB), F32),
            pltpu.SemaphoreType.DMA((BOXES_HERE,)),
        ],
        compiler_params=pltpu.CompilerParams(vmem_limit_bytes=9 << 20),
        cost_estimate=pl.CostEstimate(flops=1 << 30, bytes_accessed=7 << 20, transcendentals=0),
        name="near_fields",
    )(first_box, neighbours, counts, excite, lower, recent, upper, in_hbm(near_mats))


def near_again_kernel(
    first_box_ref, nb_ref, lower_ref, own_ref, upper_ref, before_ref, mats_ref, out_ref, win_ref
):
    box = pl.program_id(0)

    @pl.when(box == 0)
    def _():
        for place, ref in enumerate((lower_ref, own_ref, upper_ref)):
            win_ref[place * BOXES_HERE : (place + 1) * BOXES_HERE, :] = ref[...]

    total = jnp.zeros((128, 128), F32)
    for j in range(NB):
        place = nb_ref[box, j] - first_box_ref[0] + BOXES_HERE
        total = total + mats_ref[0, j, 0] * win_ref[pl.ds(place, 1), :]
    out_ref[pl.ds(box, 1), :] = before_ref[pl.ds(box + BOXES_HERE, 1), :] - row_of_sums(total)
    out_ref[pl.ds(box + 2 * BOXES_HERE, 1), :] = before_ref[pl.ds(box + 2 * BOXES_HERE, 1), :]


def near_again(first_box, neighbours, lower, own, upper, before, near_mats):
    smem = pl.BlockSpec(memory_space=pltpu.SMEM)
    side = pl.BlockSpec((BOXES_HERE, PB), lambda i: (0, 0))
    return pl.pallas_call(
        near_again_kernel,
        grid=(BOXES_HERE,),
        in_specs=[
            smem,
            smem,
            side,
            side,
            side,
            pl.BlockSpec((16, PB), lambda i: (0, 0)),
            pl.BlockSpec((1, NB, 1, PB, PB), lambda i: (i, 0, 0, 0, 0)),
        ],
        out_specs=pl.BlockSpec((16, PB), lambda i: (0, 0)),
        out_shape=jax.ShapeDtypeStruct((16, PB), F32),
        scratch_shapes=[VMEM((16, PB), F32)],
        compiler_params=pltpu.CompilerParams(vmem_limit_bytes=6 << 20),
        cost_estimate=pl.CostEstimate(flops=1 << 29, bytes_accessed=3 << 20, transcendentals=0),
        name="near_again",
    )(first_box, neighbours, lower, own, upper, before, in_hbm(near_mats))


def far_of_block(samp_ref, rows, rad, sums, ones):
    eye = identity_mask()
    for tile in range(BLOCK // 128):
        row = samp_ref[pl.ds(rows + tile, 1), :]
        high = row.astype(BF16).astype(F32)
        low = row - high
        spread = jnp.concatenate(
            [jnp.where(eye, high, 0.0).astype(BF16), jnp.where(eye, low, 0.0).astype(BF16)], axis=1
        )
        copies = jnp.dot(spread, ones, preferred_element_type=F32)
        for box in range(BOXES_HERE):
            product = rad(box, tile) * copies
            sums[box] = sums[box] + jnp.sum(product.reshape(16, 8, 128), axis=0)
    return sums


def solve(near_ref, inverse_ref, right_side, box):
    solved = row_of_sums(inverse_ref[box] * right_side)
    live = near_ref[2 * BOXES_HERE + box : 2 * BOXES_HERE + box + 1, :] > 0.5
    return jnp.where(live, solved, 0.0)


def far_of_all(samp_ref, parts_ref, rad_hbm, rad_ref, sems):
    for i in range(AHEAD_FAR):
        block_copy(rad_hbm, rad_ref, sems, i).start()
    samp_ref[...] = jnp.sum(parts_ref[...], axis=0)
    ones = jnp.ones((256, 128), BF16)

    def block(i, sums):
        first_line = pl.multiple_of(i * BLOCK, BLOCK)
        await_block(rad_hbm, rad_ref, sems, i, AHEAD_FAR)
        rad = lambda box, tile: rad_ref[
            box, pl.ds(pl.multiple_of(first_line + tile * 128, 128), 128), :
        ]
        return tuple(far_of_block(samp_ref, i * 8, rad, list(sums), ones))

    zero = jnp.zeros((8, 128), F32)
    return lax.fori_loop(0, STEPS_D, block, (zero,) * BOXES_HERE)


def first_step_kernel(
    parts_ref, near_ref, inverse_ref, second_ref, weight_ref, rad_hbm,
    current_ref, field_ref, rad_ref, samp_ref, dot_ref, sems,
):
    sums = far_of_all(samp_ref, parts_ref, rad_hbm, rad_ref, sems)
    ones = jnp.ones((256, 128), BF16)
    currents = []
    for box in range(BOXES_HERE):
        far = jnp.sum(sums[box], axis=0, keepdims=True)
        right_side = near_ref[box : box + 1, :] - far
        current = solve(near_ref, inverse_ref, right_side, box)
        current_ref[box : box + 1, :] = current
        currents.append(current)
    eye = identity_mask()

    def one_block(i, _):
        for tile in range(BLOCK // 128):
            start = pl.multiple_of(i * BLOCK + tile * 128, 128)
            product = rad_ref[0, pl.ds(start, 128), :] * currents[0]
            for box in range(1, BOXES_HERE):
                product = product + rad_ref[box, pl.ds(start, 128), :] * currents[box]
            high, low = split_two(product)
            copies_of = jnp.dot(
                jnp.concatenate([high, low], axis=1), ones, preferred_element_type=F32
            )
            dot_ref[tile : tile + 1, :] = jnp.sum(
                jnp.where(eye, copies_of, 0.0), axis=0, keepdims=True
            )
        response = dot_ref[...]
        rows = pl.ds(pl.multiple_of(i * 8, 8), 8)
        for target in range(CLUSTERS):
            field_ref[target, rows, :] = (
                second_ref[target, rows, :] + weight_ref[target, rows, :] * response
            )
        return 0

    lax.fori_loop(0, STEPS_D, one_block, 0)


def first_step(parts, near, self_inverse, second, weight, radiation):
    vmem = pl.BlockSpec(memory_space=VMEM)
    return pl.pallas_call(
        first_step_kernel,
        in_specs=[vmem] * 5 + [pl.BlockSpec(memory_space=pltpu.HBM)],
        out_specs=[vmem, vmem],
        out_shape=[
            jax.ShapeDtypeStruct((BOXES_HERE, PB), F32),
            jax.ShapeDtypeStruct((CLUSTERS, ROWS, 128), F32),
        ],
        scratch_shapes=[
            VMEM(radiation.shape, F32),
            VMEM((ROWS, 128), F32),
            VMEM((8, 128), F32),
            pltpu.SemaphoreType.DMA((STEPS_D,)),
        ],
        compiler_params=pltpu.CompilerParams(vmem_limit_bytes=28 << 20),
        cost_estimate=pl.CostEstimate(flops=4 << 30, bytes_accessed=20 << 20, transcendentals=0),
        name="first_step",
    )(parts, near, self_inverse, second, weight, in_hbm(radiation))


def second_step_kernel(
    parts_ref, near_ref, inverse_ref, before_ref, rad_hbm,
    out_ref, rad_ref, samp_ref, sems,
):
    sums = far_of_all(samp_ref, parts_ref, rad_hbm, rad_ref, sems)
    for box in range(BOXES_HERE):
        lanes = slice(box * PB, (box + 1) * PB)
        far = jnp.sum(sums[box], axis=0, keepdims=True)
        right_side = near_ref[box : box + 1, :] - far
        out_ref[0:1, lanes] = before_ref[box : box + 1, :]
        out_ref[1:2, lanes] = solve(near_ref, inverse_ref, right_side, box)


def second_step(parts, near, self_inverse, before, radiation):
    vmem = pl.BlockSpec(memory_space=VMEM)
    return pl.pallas_call(
        second_step_kernel,
        in_specs=[vmem] * 4 + [pl.BlockSpec(memory_space=pltpu.HBM)],
        out_specs=vmem,
        out_shape=jax.ShapeDtypeStruct((STEPS, BOXES_HERE * PB), F32),
        scratch_shapes=[
            VMEM(radiation.shape, F32),
            VMEM((ROWS, 128), F32),
            pltpu.SemaphoreType.DMA((STEPS_D,)),
        ],
        compiler_params=pltpu.CompilerParams(vmem_limit_bytes=28 << 20),
        cost_estimate=pl.CostEstimate(flops=4 << 30, bytes_accessed=20 << 20, transcendentals=0),
        name="second_step",
    )(parts, near, self_inverse, before, in_hbm(radiation))


def from_behind(array, by):
    axis = ("space", "ray")
    size = lax.axis_size(axis)
    pairs = [(i, i + by) for i in range(size) if 0 <= i + by < size]
    return lax.ppermute(array, axis, pairs)


def sum_kernel(arrived_ref, copies_ref):
    total = jnp.sum(arrived_ref[...], axis=0)
    for copy in range(copies_ref.shape[0]):
        copies_ref[copy] = total


def summed_copies(arrived, copies):
    vmem = pl.BlockSpec(memory_space=VMEM)
    return pl.pallas_call(
        sum_kernel,
        in_specs=[vmem],
        out_specs=vmem,
        out_shape=jax.ShapeDtypeStruct((copies, *arrived.shape[1:]), F32),
        compiler_params=pltpu.CompilerParams(vmem_limit_bytes=4 << 20),
        cost_estimate=pl.CostEstimate(flops=1 << 17, bytes_accessed=1 << 20, transcendentals=0),
        name="summed_copies",
    )(arrived)


def over_clusters(field):
    return lax.all_to_all(field, "space", split_axis=0, concat_axis=0, tiled=True)


def over_rays(copies):
    return lax.all_to_all(copies, "ray", split_axis=0, concat_axis=0, tiled=True)


def steps(
    excite, history, near_mats, neighbours, self_inverse, radiation, directions, centers, counts
):
    space = lax.axis_index("space").astype(jnp.int32).reshape(1)
    first_box = (lax.axis_index(("space", "ray")) * BOXES_HERE).astype(jnp.int32).reshape(1)
    ray_size = lax.axis_size("ray")
    first, out, twice, scale, recent = translate(space, centers, history, directions, radiation)
    upper = from_behind(recent, -1)
    second, weight = known_part(space, out, twice, scale)
    copies = summed_copies(over_clusters(first), ray_size)
    copies, upper, second, weight, recent = lax.optimization_barrier(
        (copies, upper, second, weight, recent)
    )
    parts = over_rays(copies)
    lower = from_behind(recent, 1)
    near = near_fields(
        first_box, neighbours, counts, excite, lower, recent, upper, near_mats
    )
    current, field = first_step(parts, near, self_inverse, second, weight, radiation)
    upper = from_behind(current, -1)
    copies = summed_copies(over_clusters(field), ray_size)
    copies, upper, current = lax.optimization_barrier((copies, upper, current))
    parts = over_rays(copies)
    lower = from_behind(current, 1)
    near = near_again(first_box, neighbours, lower, current, upper, near, near_mats)
    return second_step(parts, near, self_inverse, current, radiation)


def solution(mesh):
    placed = (
        P(None, ("space", "ray")),
        P(None, ("space", "ray")),
        P(("space", "ray"), None, None, None, None),
        P(("space", "ray"), None),
        P(("space", "ray"), None, None),
        P(("space", "ray"), None, None),
        P(),
        P(),
        P(("space", "ray")),
    )
    return jax.shard_map(
        steps, mesh=mesh, in_specs=placed, out_specs=P(None, ("space", "ray")), check_vma=False
    )
```
